256 devices in a mesh: gx: 4 (over y), gy: 8 (over x, core), gz: 8 (over z).
Axes of the slice: x: 4, y: 4, z: 8, core: 2. Of those that a mesh axis runs over, the one named last changes fastest.
Arguments:
- flow_state: float32 [5, 256, 128, 512], P(None, 'gz', 'gy', 'gx'), may hold values from -5 to 120, as said below
- advection: float32 [3, 5], replicated, may hold values from -400 to 400, as said below
- inverse_x: float32 [5, 128, 128], replicated, may hold values from -1 to 1, as said below
- inverse_y: float32 [5, 16, 16], replicated, may hold values from -1 to 1, as said below
- inverse_z: float32 [5, 32, 32], replicated, may hold values from -1 to 1, as said below
- reduced_x: float32 [5, 16, 16], replicated, as said below
- reduced_y: float32 [5, 32, 32], replicated, as said below
- reduced_z: float32 [5, 32, 32], replicated, as said below
Outputs:
- update: float32 [5, 256, 128, 512], P(None, 'gz', 'gy', 'gx')
- rms_norm: float32 [5], replicated
The draws below stay inside these ranges and needn't reach their ends.
Inputs may be any that keep to these rules, and one draw needn't show every extreme that they name: flow_state[0] (density) lies between 0.5 and 2, and flow_state[4] / density minus half the squared velocity is at least 0.6 in every cell. `advection`: every entry has magnitude between 100 and 400. inverse_x[v] is the inverse of the 128 x 128 matrix with 4 on the diagonal, advection[0, v] / 2 - 2 just above it, -advection[0, v] / 2 - 2 just below it and 0.5 two places off it. inverse_y[v] is the inverse of the 16 x 16 matrix built likewise from advection[1, v]. inverse_z[v] is the inverse of the 32 x 32 matrix built likewise from advection[2, v]. reduced_x[v] is the inverse of I + K, K being the boundary rows and columns of the block inverses times the coupling between blocks, so that S_x equals the exact solution of the banded system along whole x lines with nothing beyond the grid's ends. reduced_y[v] is built likewise for y lines. reduced_z[v] is built likewise for z lines.
All inputs are finite; a program needn't handle non-finite values.
Results may differ from the reference program's by a relative error of at most 0.0002.
Values sent between devices are 32-bit elements.
No kernel may reach another device: no remote copies, remote signals or barrier semaphores. Data moves between devices by JAX's collectives and lax.ppermute only.
A program may use at most 64 MiB of HBM per device.

```python
import jax
import jax.numpy as jnp
import numpy as np
from jax import lax

VARS = 5
CX = 128
CY = 16
CZ = 32
NX = 512
NY = 128
NZ = 256


fourth_coef = 0.5


def advection_table(key):
    subkeys = jax.random.split(jax.random.fold_in(key, 17), 2)
    magnitude = 100.0 * 4.0 ** jax.random.uniform(subkeys[0], (3, VARS), jnp.float32)
    signs = 2.0 * jax.random.randint(subkeys[1], (3, VARS), 0, 2).astype(jnp.float32) - 1.0
    return signs * magnitude


def band_matrix(length, speed):
    identity = jnp.eye(length, dtype=jnp.float32)
    upper_band = jnp.eye(length, k=1, dtype=jnp.float32)
    lower_band = jnp.eye(length, k=-1, dtype=jnp.float32)
    second_band = jnp.eye(length, k=2, dtype=jnp.float32) + jnp.eye(length, k=-2, dtype=jnp.float32)
    return (1.0 + 6.0 * fourth_coef) * identity + (0.5 * speed - 4.0 * fourth_coef) * upper_band + (-0.5 * speed - 4.0 * fourth_coef) * lower_band + fourth_coef * second_band


def block_inverse(key, direction, block_len):
    speeds = advection_table(key)[direction]
    return jax.vmap(lambda speed: jnp.linalg.inv(band_matrix(block_len, speed)))(speeds)


def reduced_inverse(key, direction, block_len, blocks):
    speeds = advection_table(key)[direction]
    length = block_len * blocks
    picked = (block_len * np.arange(blocks)[:, None] + np.array([0, 1, block_len - 2, block_len - 1])[None, :]).reshape(-1)

    def single(speed):
        local_block = band_matrix(block_len, speed)
        whole_line = band_matrix(length, speed)
        spread_inv = jnp.kron(jnp.eye(blocks, dtype=jnp.float32), jnp.linalg.inv(local_block))
        coupling = whole_line - jnp.kron(jnp.eye(blocks, dtype=jnp.float32), local_block)
        product = jnp.dot(spread_inv, coupling, precision=lax.Precision.HIGHEST)
        reduced_k = product[picked][:, picked]
        return jnp.linalg.inv(jnp.eye(4 * blocks, dtype=jnp.float32) + reduced_k)
    return jax.vmap(single)(speeds)


def region_envelope(key):
    phases = jax.random.uniform(jax.random.fold_in(key, 29), (2,), jnp.float32, 0.0, 6.2831853)
    along_z = jnp.arange(NZ, dtype=jnp.float32) * (6.2831853 / NZ)
    along_y = jnp.arange(NY, dtype=jnp.float32) * (6.2831853 / NY)
    shape_z = 0.5 + 0.5 * jnp.sin(along_z + phases[0])
    shape_y = 0.5 + 0.5 * jnp.cos(along_y + phases[1])
    envelope = 0.2 + 0.8 * shape_z[:, None] * shape_y[None, :]
    return envelope[:, :, None]


def draw_flow_state(key, part):
    subkeys = jax.random.split(jax.random.fold_in(key, 11), 6)
    grid_shape = (NZ, NY, NX)
    envelope = region_envelope(key)
    density = 0.5 * 4.0 ** jax.random.uniform(subkeys[0], grid_shape, jnp.float32)
    velocity = jnp.clip(0.6 * jax.random.normal(subkeys[1], (3,) + grid_shape, jnp.float32), -2.5, 2.5)
    baseline = jax.random.uniform(subkeys[2], grid_shape, jnp.float32, 0.6, 1.8)
    density = 1.0 + envelope * (density - 1.0)
    velocity = envelope[None] * velocity
    baseline = 0.6 + envelope * (baseline - 0.6)
    cell_total = NZ * NY * NX
    segment = cell_total // 8
    offsets = jax.random.randint(subkeys[3], (8,), 0, segment)
    hot_cells = jnp.arange(8, dtype=jnp.int32) * segment + offsets
    ranking = jax.random.permutation(subkeys[4], 8)
    levels = 10.0 * 1.25 ** ranking.astype(jnp.float32)
    hot_extra = jnp.zeros((cell_total,), jnp.float32).at[hot_cells].add(levels).reshape(grid_shape)
    internal = baseline + hot_extra
    momentum = density * velocity
    energy = density * (internal + 0.5 * jnp.sum(velocity * velocity, axis=0))
    return jnp.stack([density, momentum[0], momentum[1], momentum[2], energy])


def draw_advection(key, part):
    return advection_table(key)


def draw_inverse_x(key, part):
    return block_inverse(key, 0, CX)


def draw_inverse_y(key, part):
    return block_inverse(key, 1, CY)


def draw_inverse_z(key, part):
    return block_inverse(key, 2, CZ)


def draw_reduced_x(key, part):
    return reduced_inverse(key, 0, CX, NX // CX)


def draw_reduced_y(key, part):
    return reduced_inverse(key, 1, CY, NY // CY)


def draw_reduced_z(key, part):
    return reduced_inverse(key, 2, CZ, NZ // CZ)


def setup_inputs(seed: int = 0) -> dict:
    arg_keys = jax.random.split(jax.random.key(seed), 9)
    return {
        "flow_state": draw_flow_state(jax.random.fold_in(arg_keys[8], 71), 0),
        "advection": draw_advection(jax.random.fold_in(arg_keys[8], 71), 0),
        "inverse_x": draw_inverse_x(jax.random.fold_in(arg_keys[8], 71), 0),
        "inverse_y": draw_inverse_y(jax.random.fold_in(arg_keys[8], 71), 0),
        "inverse_z": draw_inverse_z(jax.random.fold_in(arg_keys[8], 71), 0),
        "reduced_x": draw_reduced_x(jax.random.fold_in(arg_keys[8], 71), 0),
        "reduced_y": draw_reduced_y(jax.random.fold_in(arg_keys[8], 71), 0),
        "reduced_z": draw_reduced_z(jax.random.fold_in(arg_keys[8], 71), 0),
    }


exact_mode = lax.Precision.HIGHEST
gas_ratio = 0.4
courant = 8000.0
damping = 0.0625
fourth_coef = 0.5

def primitives(flow_state):
    density = flow_state[0]
    velocity = flow_state[1:4] / density
    kinetic = 0.5 * lax.optimization_barrier(jnp.sum(velocity * velocity, axis=0))
    internal = jnp.maximum(flow_state[4] / density - kinetic, 0.25)
    pressure = gas_ratio * density * internal
    return (velocity, internal, pressure)

def flux_component(flow_state, velocity, pressure, variable, direction):
    carried = velocity[direction]
    if variable == 0:
        return flow_state[1 + direction]
    if variable < 4:
        moment = flow_state[variable] * carried
        if variable - 1 == direction:
            moment = moment + pressure
        return moment
    return (flow_state[4] + pressure) * carried

def residual_field(flow_state, velocity, pressure):
    collected = []
    for variable in range(VARS):
        field = flow_state[variable]
        running = jnp.zeros_like(field)
        for direction in range(3):
            line_axis = 2 - direction
            flux = flux_component(flow_state, velocity, pressure, variable, direction)
            running = running - 0.5 * (jnp.roll(flux, -1, line_axis) - jnp.roll(flux, 1, line_axis))
            fourth = jnp.roll(field, 2, line_axis) - 4.0 * jnp.roll(field, 1, line_axis) + 6.0 * field - 4.0 * jnp.roll(field, -1, line_axis) + jnp.roll(field, -2, line_axis)
            running = running - damping * fourth
        collected.append(running)
    return jnp.stack(collected)

def neighbour_table(reduced):
    blocks = reduced.shape[0] // 4
    padded = jnp.pad(reduced, ((2, 2), (0, 0)))
    picked = (4 * np.arange(blocks)[:, None] + np.array([0, 1, 6, 7])[None, :]).reshape(-1)
    return padded[picked]

def line_solve(line_field, line_axis, inverse, reduced, speed):
    moved = jnp.moveaxis(line_field, line_axis, -1)
    block_len = inverse.shape[0]
    blocks = reduced.shape[0] // 4
    leading = moved.shape[:-1]
    split = moved.reshape(leading + (blocks, block_len))
    local_part = jnp.einsum('ij,abpj->abpi', inverse, split, precision=exact_mode)
    boundary = jnp.stack([local_part[..., 0], local_part[..., 1], local_part[..., block_len - 2], local_part[..., block_len - 1]], axis=-1).reshape(leading + (4 * blocks,))
    nearby = jnp.einsum('rq,abq->abr', neighbour_table(reduced), boundary, precision=exact_mode).reshape(leading + (blocks, 4))
    lower_one = -0.5 * speed - 4.0 * fourth_coef
    upper_one = 0.5 * speed - 4.0 * fourth_coef
    left_first = fourth_coef * nearby[..., 0] + lower_one * nearby[..., 1]
    left_second = fourth_coef * nearby[..., 1]
    right_first = fourth_coef * nearby[..., 2]
    right_second = upper_one * nearby[..., 2] + fourth_coef * nearby[..., 3]
    correction = inverse[:, 0] * left_first[..., None] + inverse[:, 1] * left_second[..., None] + inverse[:, block_len - 2] * right_first[..., None] + inverse[:, block_len - 1] * right_second[..., None]
    solved = (local_part - correction).reshape(moved.shape)
    return jnp.moveaxis(solved, -1, line_axis)

def reference(flow_state, advection, inverse_x, inverse_y, inverse_z, reduced_x, reduced_y, reduced_z):
    velocity, internal, pressure = primitives(flow_state)
    wave_speed = lax.optimization_barrier(jnp.sum(jnp.abs(velocity), axis=0)) + jnp.sqrt(3.0 * 1.4 * gas_ratio * internal)
    top_speed = jnp.max(wave_speed)
    time_step = courant / top_speed
    residual = residual_field(flow_state, velocity, pressure)
    rms_norm = jnp.sqrt(lax.optimization_barrier(jnp.sum(residual * residual, axis=(1, 2, 3))) / (NX * NY * NZ))
    inverses = (inverse_x, inverse_y, inverse_z)
    reduceds = (reduced_x, reduced_y, reduced_z)
    collected = []
    for variable in range(VARS):
        line_field = time_step * residual[variable]
        for direction in range(3):
            line_field = line_solve(line_field, 2 - direction, inverses[direction][variable], reduceds[direction][variable], advection[direction, variable])
        collected.append(line_field)
    return (jnp.stack(collected), rms_norm)
```

```python
import functools

import jax
import jax.numpy as jnp
from jax import lax
from jax.experimental import pallas as pl
from jax.experimental.pallas import tpu as pltpu
from jax.sharding import PartitionSpec as P

VARS = 5
F32 = jnp.float32
BF16 = jnp.bfloat16
DAMP = 0.0625
COURANT = 8000.0
VMEM = pltpu.VMEM
NN = (((1,), (0,)), ((), ()))
NT = (((1,), (1,)), ((), ()))


def iota(shape, dim):
    return lax.broadcasted_iota(jnp.int32, shape, dim)


def picks(shape, cond):
    return jnp.where(cond(iota(shape, 0), iota(shape, 1)), 1.0, 0.0).astype(BF16)


def split(x):
    hi = x.astype(BF16)
    return hi, (x - hi.astype(F32)).astype(BF16)


def dot1(a, b, dims=NN):
    return lax.dot_general(a, b, dims, preferred_element_type=F32)


def dot3(a, b, dims=NN):
    return dot1(a[0], b[0], dims) + (dot1(a[0], b[1], dims) + dot1(a[1], b[0], dims))


def call(body, out, args, scratch=(), smem=0, flops=1_000_000):
    specs = [pl.BlockSpec(memory_space=pltpu.SMEM)] * smem
    specs += [pl.BlockSpec(memory_space=VMEM)] * (len(args) - smem)
    size = sum(a.size * a.dtype.itemsize for a in args)
    return pl.pallas_call(
        body,
        out_shape=[jax.ShapeDtypeStruct(*o) for o in out],
        in_specs=specs,
        out_specs=[pl.BlockSpec(memory_space=VMEM)] * len(out),
        scratch_shapes=[VMEM(*s) for s in scratch],
        compiler_params=pltpu.CompilerParams(vmem_limit_bytes=36 * 1024 * 1024),
        cost_estimate=pl.CostEstimate(flops=flops, bytes_accessed=size, transcendentals=0),
    )(*args)


def tables_body(adv, idx, invx, invy, invz, redx, redy, redz, ax, qx, ay, qy, az, qz, qzy, nx, my, mz):
    ix = idx[0]
    nx[...] = jnp.zeros_like(nx)

    def spread(left, parts, right, keep, write):
        for k, part in enumerate(parts):
            wide = dot1(dot1(left, part).astype(BF16), right)
            write(k, (jnp.where(keep, wide, 0.0) if keep is not None else wide).astype(BF16))

    def masked(shape, cond):
        return cond(iota(shape, 0), iota(shape, 1))

    def near(red, speed):
        rows = red.shape[0]
        i, k = iota((rows, rows), 0), iota((rows, rows), 1)
        r, d = i & 3, k - (i - (i & 3))
        lower, upper = -0.5 * speed - 2.0, 0.5 * speed - 2.0
        half = jnp.where(
            ((r == 0) & (d == -2)) | ((r == 1) & (d == -1)) | ((r == 2) & (d == 4)) | ((r == 3) & (d == 5)),
            0.5,
            0.0,
        )
        other = jnp.where((r == 0) & (d == -1), lower, jnp.where((r == 3) & (d == 4), upper, 0.0))
        return lax.dot_general(half + other, red, NN, precision=lax.Precision.HIGHEST, preferred_element_type=F32)

    def per_variable(v, carry):
        parts = split(invx[v])
        pick = picks((128, 128), lambda a, c: ((a >> 2) == v) & (c == ((126 + (a & 3)) & 127)))
        for k in range(2):
            ax[2 * v + k] = parts[k]
            qx[2 * v + k] = dot1(pick, parts[k], NT).astype(BF16)

        def put(ref):
            def write(k, value):
                ref[2 * v + k] = value

            return write

        parts = split(invy[v])
        spread(
            picks((128, 16), lambda a, k: (a & 15) == k),
            parts,
            picks((16, 128), lambda k, c: k == (c & 15)),
            masked((128, 128), lambda a, c: (a >> 4) == (c >> 4)),
            put(ay),
        )
        spread(
            picks((512, 16), lambda a, k: (a & 15) == k),
            parts,
            picks((16, 128), lambda k, c: k == (c & 3) + 12 * ((c & 3) >> 1)),
            masked((512, 128), lambda a, c: (((a >> 4) & 7) == (c >> 4)) & ((a >> 7) == ((c >> 2) & 3))),
            put(qy),
        )
        parts = split(invz[v])
        left = picks((256, 32), lambda a, k: (a >> 3) == k)
        spread(
            left,
            parts,
            picks((32, 256), lambda k, c: k == (c >> 3)),
            masked((256, 256), lambda a, c: (a & 7) == (c & 7)),
            put(az),
        )
        spread(
            left,
            parts,
            picks((32, 32), lambda k, c: k == (c >> 3) + 28 * (c >> 4)),
            masked((256, 32), lambda a, c: (a & 7) == (c & 7)),
            put(qz),
        )
        spread(
            picks((128, 32), lambda a, k: k == ((a >> 2) & 3) * 8 + (a >> 4)),
            parts,
            picks((32, 16), lambda k, c: k == (c >> 2) + 28 * (c >> 3)),
            masked((128, 16), lambda a, c: (a & 3) == (c & 3)),
            put(qzy),
        )
        parts = split(near(redy[v], adv[1, v]))
        spread(
            picks((128, 32), lambda a, k: k == 4 * (a >> 4) + (a & 3)),
            parts,
            picks((32, 128), lambda k, c: k == 4 * (c >> 4) + (c & 3)),
            masked((128, 128), lambda a, c: ((a >> 2) & 3) == ((c >> 2) & 3)),
            put(my),
        )
        parts = split(near(redz[v], adv[2, v]))
        spread(
            picks((64, 32), lambda a, k: k == 4 * (a >> 3) + (a & 3)),
            parts,
            picks((32, 64), lambda k, c: k == 4 * (c >> 3) + (c & 3)),
            masked((64, 64), lambda a, c: ((a >> 2) & 1) == ((c >> 2) & 1)),
            put(mz),
        )
        parts = split(near(redx[v], adv[0, v]))
        left = picks((32, 16), lambda a, k: ((a >> 2) == v) & (k == 4 * ix + ((a & 3) ^ 2)))
        for s in range(4):
            peer = (ix + 4 - s) & 3

            def add(k, value, s=s):
                nx[2 * s + k] += value

            spread(
                left,
                parts,
                picks((16, 32), lambda k, c: ((c >> 2) == v) & (k == 4 * peer + ((c & 3) ^ 2))),
                None,
                add,
            )
        return carry

    lax.fori_loop(0, VARS, per_variable, 0)


def tables(idx, advection, *small):
    shapes = [
        (10, 128, 128),
        (10, 128, 128),
        (10, 128, 128),
        (10, 512, 128),
        (10, 256, 256),
        (10, 256, 32),
        (10, 128, 16),
        (8, 32, 32),
        (10, 128, 128),
        (10, 64, 64),
    ]
    return call(
        tables_body, [(s, BF16) for s in shapes], (advection, idx, *small), smem=2, flops=20_000_000
    )


def faces_body(u, xlo, xhi, ylo, yhi, zlo, zhi):
    lane = iota((512, 128), 1)
    wide = jnp.zeros((512, 128), F32)
    for v in range(VARS):
        block = u[512 * v : 512 * v + 512, :]
        low = pltpu.roll(block, 2 * v, 1) if v else block
        wide = jnp.where((lane >> 1) == v, low, wide)
        wide = jnp.where((lane >> 1) == 8 + v, pltpu.roll(block, 18 + 2 * v, 1), wide)
        for j in range(2):
            at = 32 * (2 * v + j)
            ylo[at : at + 32, :] = u[pl.ds(512 * v + j, 32, stride=16), :]
            yhi[at : at + 32, :] = u[pl.ds(512 * v + 14 + j, 32, stride=16), :]
        zlo[32 * v : 32 * v + 32, :] = u[512 * v : 512 * v + 32, :]
        zhi[32 * v : 32 * v + 32, :] = u[512 * v + 480 : 512 * v + 512, :]
    turned = wide.T
    xlo[...] = turned[0:16]
    xhi[...] = turned[16:32]


def primitives(u):
    inverse = 1.0 / u[0]
    velocity = [u[1 + k] * inverse for k in range(3)]
    kinetic = 0.5 * (velocity[0] * velocity[0] + velocity[1] * velocity[1] + velocity[2] * velocity[2])
    internal = jnp.maximum(u[4] * inverse - kinetic, 0.25)
    return velocity, internal, 0.4 * u[0] * internal


def flux(u, velocity, pressure, d):
    w = velocity[d]
    out = [u[1 + d]]
    for k in range(3):
        moment = u[1 + k] * w
        out.append(moment + pressure if k == d else moment)
    out.append((u[4] + pressure) * w)
    return out


def stats_row(shape, sums, top):
    lane = iota(shape, len(shape) - 1)
    row = jnp.where(lane == VARS, top, 0.0)
    for v in range(VARS):
        row = jnp.where(lane == v, sums[v], row)
    return row


def merged_stats(rows):
    lane = iota(rows[0].shape, 1)
    total, top = rows[0], rows[0]
    for row in rows[1:]:
        total, top = total + row, jnp.maximum(top, row)
    return jnp.where(lane < VARS, total, top)


def residual_body(
    u, xlo, xhi, ylo, yhi, zlo, zhi, own_lo, own_hi, ax, ay, az, w, bx, pad, fy, fz, res, fix, half, edge
):
    def fill(z, carry):
        for v in range(VARS):
            pad[36 * v + 2 + z, 8:24, :] = u[pl.ds(pl.multiple_of(512 * v + 16 * z, 16), 16), :]
        return carry

    lax.fori_loop(0, 32, fill, 0)
    rows = pad.reshape(180 * 32, 128)
    for v in range(VARS):
        for k in range(2):
            pad[36 * v + k, 8:24, :] = zlo[32 * v + 16 * k : 32 * v + 16 * k + 16, :]
            pad[36 * v + 34 + k, 8:24, :] = zhi[32 * v + 16 * k : 32 * v + 16 * k + 16, :]
            at = 32 * (2 * v + k)
            rows[pl.ds(32 * (36 * v + 2) + 6 + k, 32, stride=32), :] = ylo[at : at + 32, :]
            rows[pl.ds(32 * (36 * v + 2) + 24 + k, 32, stride=32), :] = yhi[at : at + 32, :]

    edge[...] = jnp.zeros_like(edge)

    def line(ref, j):
        return [ref[2 * v + j : 2 * v + j + 1, :] for v in range(VARS)]

    def fx(u):
        velocity, _, pressure = primitives(u)
        return flux(u, velocity, pressure, 0)

    l2, l1, h1, h2 = line(xlo, 0), line(xlo, 1), line(xhi, 0), line(xhi, 1)
    o0, o1, p1, p0 = line(own_lo, 0), line(own_lo, 1), line(own_hi, 0), line(own_hi, 1)
    fl, fp, fh, fo = fx(l1), fx(p0), fx(h1), fx(o0)
    for v in range(VARS):
        dl, dh = l1[v] - p0[v], h1[v] - o0[v]
        edge[4 * v : 4 * v + 1, :] = -DAMP * dh
        edge[4 * v + 1 : 4 * v + 2, :] = -0.5 * (fh[v] - fo[v]) + 4.0 * DAMP * dh - DAMP * (h2[v] - o1[v])
        edge[4 * v + 2 : 4 * v + 3, :] = 0.5 * (fl[v] - fp[v]) + 4.0 * DAMP * dl - DAMP * (l2[v] - p1[v])
        edge[4 * v + 3 : 4 * v + 4, :] = -DAMP * dl
    fix[...] = edge[...].T

    for z in (-1, 32):
        c = [pad[36 * v + 2 + z, 8:24, :] for v in range(VARS)]
        velocity, _, pressure = primitives(c)
        for v, f in enumerate(flux(c, velocity, pressure, 2)):
            fz[34 * v + 1 + z] = f

    def plane(z, top):
        full = [pad[36 * v + 2 + z] for v in range(VARS)]
        velocity, internal, pressure = primitives(full)
        for v, f in enumerate(flux(full, velocity, pressure, 1)):
            fy[32 * v + z] = f
        c = [f[8:24] for f in full]
        velocity, internal, pressure = [f[8:24] for f in velocity], internal[8:24], pressure[8:24]
        for v, f in enumerate(flux(c, velocity, pressure, 2)):
            fz[34 * v + 1 + z] = f
        for v, f in enumerate(flux(c, velocity, pressure, 0)):
            damped = (4.0 * DAMP) * c[v]
            res[32 * v + z] = (
                pltpu.roll(damped - 0.5 * f, 127, 1)
                + pltpu.roll(damped + 0.5 * f, 1, 1)
                - DAMP * (pltpu.roll(c[v], 126, 1) + pltpu.roll(c[v], 2, 1))
                - (18.0 * DAMP) * c[v]
            )
        speed = jnp.abs(velocity[0]) + jnp.abs(velocity[1]) + jnp.abs(velocity[2])
        return jnp.maximum(top, speed + jnp.sqrt((3.0 * 1.4 * 0.4) * internal))

    top = lax.fori_loop(0, 32, plane, jnp.zeros((16, 128), F32))

    lane = iota((16, 128), 1)
    edges = (lane < 2) | (lane >= 126)

    def finish(z, sums):
        out = []
        fixes = fix[pl.ds(pl.multiple_of(16 * z, 16), 16), :]
        for v in range(VARS):
            at = 36 * v + 2 + z
            ones = (pad[at, 7:23, :] + pad[at, 9:25, :]) + (pad[at - 1, 8:24, :] + pad[at + 1, 8:24, :])
            twos = (pad[at, 6:22, :] + pad[at, 10:26, :]) + (pad[at - 2, 8:24, :] + pad[at + 2, 8:24, :])
            steep = (fy[32 * v + z, 7:23, :] - fy[32 * v + z, 9:25, :]) + (fz[34 * v + z] - fz[34 * v + 2 + z])
            value = res[32 * v + z] + 0.5 * steep + (4.0 * DAMP) * ones - DAMP * twos
            value = value + jnp.where(edges, pltpu.roll(fixes, (126 - 4 * v) & 127, 1), 0.0)
            res[32 * v + z] = value
            out.append(sums[v] + value * value)
        return tuple(out)

    sums = lax.fori_loop(0, 32, finish, tuple(jnp.zeros((16, 128), F32) for _ in range(VARS)))

    def solve(v, carry):
        field = res[pl.ds(32 * v, 32)].reshape(512, 128)
        half[...] = dot3(split(field), (ax[2 * v], ax[2 * v + 1]), NT)
        table = (ay[2 * v], ay[2 * v + 1])
        for g in range(4):
            half[128 * g : 128 * g + 128, :] = dot3(table, split(half[128 * g : 128 * g + 128, :]))
        table = (az[2 * v], az[2 * v + 1])
        field = half[...].reshape(32, 2, 8, 128)
        parts = [dot3(table, split(field[:, h].reshape(256, 128))).reshape(32, 1, 8, 128) for h in range(2)]
        w[pl.ds(pl.multiple_of(512 * v, 512), 512), :] = jnp.concatenate(parts, axis=1).reshape(512, 128)
        return carry

    lax.fori_loop(0, VARS, solve, 0)
    lane = iota((512, 128), 1)
    wide = jnp.zeros((512, 128), F32)
    for v in range(VARS):
        wide = jnp.where((lane >> 2) == v, pltpu.roll(w[512 * v : 512 * v + 512, :], 2 + 4 * v, 1), wide)
    turned = wide.T
    bx[...] = turned[0:24]
    bx[20:21, :] = stats_row((1, 512), [jnp.sum(s) for s in sums], jnp.max(top))


def spread_body(w, b0, b1, b2, b3, nx, qx, v1, yp, zp, wide, yb, zb):
    total = None
    blank = jnp.zeros((8, 512), F32)
    pieces = [b0, b1, b2, b3]
    for s in range(4):
        term = dot3((nx[2 * s], nx[2 * s + 1]), split(jnp.concatenate([pieces[s][...], blank], axis=0)))
        total = term if total is None else total + term
    wide[...] = jnp.zeros_like(wide)
    wide[0:32, :] = total
    turned = split(wide[...].T)

    def correct(v, carry):
        at = pl.ds(pl.multiple_of(512 * v, 512), 512)
        v1[at, :] = w[at, :] - dot3(turned, (qx[2 * v], qx[2 * v + 1]))
        return carry

    lax.fori_loop(0, VARS, correct, 0)
    for v in range(VARS):
        for t in range(4):
            for j, y in enumerate((0, 1, 14, 15)):
                at = ((v * 4 + t) * 4 + j) * 8
                yb[at : at + 8, :] = v1[pl.ds(512 * v + 128 * t + y, 8, stride=16), :]
        for h in range(2):
            for j, z in enumerate((0, 1, 30, 31)):
                at = ((v * 2 + h) * 4 + j) * 8
                zb[at : at + 8, :] = v1[512 * v + 16 * z + 8 * h : 512 * v + 16 * z + 8 * h + 8, :]
    stats = merged_stats([p[20:21, 0:128] for p in pieces])
    for p in range(8):
        yp[88 * p : 88 * p + 80, :] = yb[pl.ds(p, 80, stride=8), :]
        yp[88 * p + 80 : 88 * p + 88, :] = jnp.broadcast_to(stats, (8, 128))
        zp[40 * p : 40 * p + 40, :] = zb[pl.ds(p, 40, stride=8), :]


def owner_y_body(yr, my, yo, st):
    def one(v, carry):
        at = pl.multiple_of(16 * v, 16)
        data = jnp.concatenate([yr[pl.ds(88 * q + at, 16), :] for q in range(8)], axis=0)
        out = dot3((my[2 * v], my[2 * v + 1]), split(data))
        for p in range(8):
            yo[pl.ds(80 * p + at, 16), :] = out[16 * p : 16 * p + 16]
        return carry

    lax.fori_loop(0, VARS, one, 0)
    st[...] = merged_stats([yr[88 * q + 80 : 88 * q + 88, :] for q in range(8)])


def owner_z_body(zr, st, mz, zo):
    def one(v, carry):
        at = pl.multiple_of(8 * v, 8)
        data = jnp.concatenate([zr[pl.ds(40 * q + at, 8), :] for q in range(8)], axis=0)
        out = dot3((mz[2 * v], mz[2 * v + 1]), split(data))
        for p in range(8):
            zo[pl.ds(48 * p + at, 8), :] = out[8 * p : 8 * p + 8]
        return carry

    lax.fori_loop(0, VARS, one, 0)
    for p in range(8):
        zo[48 * p + 40 : 48 * p + 48, :] = st[...]


def cross_body(zg, zc, zy, fin):
    for v in range(VARS):
        for h in range(2):
            for r in range(4):
                at = ((v * 2 + h) * 4 + r) * 8
                zc[at : at + 8, :] = zg[pl.ds(8 * v + 4 * h + r, 8, stride=48), :]
        for j, (c, h) in enumerate(((0, 0), (1, 0), (6, 1), (7, 1))):
            zy[pl.ds(16 * v + j, 4, stride=4), :] = zg[48 * c + 8 * v + 4 * h : 48 * c + 8 * v + 4 * h + 4, :]
    for p in range(1, 8):
        zy[80 * p : 80 * p + 80, :] = zy[0:80, :]
    stats = merged_stats([zg[48 * q + 40 : 48 * q + 48, :] for q in range(8)])
    lane = iota((8, 128), 1)
    top = jnp.max(jnp.where(lane == VARS, stats, 0.0))
    norm = jnp.sqrt(stats * (1.0 / 16777216.0))
    fin[...] = jnp.where(lane == VARS, COURANT / top, norm)


def middle_body(v1, zc, yg, qz, qy, v2):
    def one(v, carry):
        base = pl.multiple_of(512 * v, 512)
        at = pl.multiple_of(16 * v, 16)
        data = jnp.concatenate([yg[pl.ds(80 * c + at, 16), :] for c in range(8)], axis=0)
        v2[pl.ds(base, 512), :] = v1[pl.ds(base, 512), :] - dot3((qy[2 * v], qy[2 * v + 1]), split(data))
        table = (qz[2 * v], qz[2 * v + 1])
        parts = []
        for h in range(2):
            rows = zc[pl.ds(pl.multiple_of(64 * v + 32 * h, 32), 32), :]
            parts.append(dot3(table, split(rows)).reshape(32, 1, 8, 128))
        v2[pl.ds(base, 512), :] -= jnp.concatenate(parts, axis=1).reshape(512, 128)
        return carry

    lax.fori_loop(0, VARS, one, 0)


def last_body(idx, v2, zr, fin, my, qzy, qy, out):
    iy = idx[1]
    lane = iota((8, 128), 1)
    step = jnp.max(jnp.where(lane == VARS, fin[...], 0.0))

    def one(v, carry):
        base = pl.multiple_of(512 * v, 512)
        at = pl.multiple_of(16 * v, 16)
        data = jnp.concatenate([zr[pl.ds(80 * q + at, 16), :] for q in range(8)], axis=0)
        mine = pl.ds(pl.multiple_of(16 * iy, 16), 16)
        crossed = dot3((my[2 * v, mine, :], my[2 * v + 1, mine, :]), split(data))
        lines = dot3((qzy[2 * v], qzy[2 * v + 1]), split(crossed))
        value = v2[pl.ds(base, 512), :] + dot3((qy[2 * v], qy[2 * v + 1]), split(lines))
        out[pl.ds(base, 512), :] = step * value
        return carry

    lax.fori_loop(0, VARS, one, 0)


def handed(x, axis):
    return lax.all_to_all(x, axis, 0, 0, tiled=True)


def shifted(x, axis, by):
    size = lax.axis_size(axis)
    return lax.ppermute(x, axis, [(i, (i + by) % size) for i in range(size)])


def shards(flow_state, advection, inverse_x, inverse_y, inverse_z, reduced_x, reduced_y, reduced_z):
    idx = jnp.stack([lax.axis_index(a) for a in ("gx", "gy", "gz")]).astype(jnp.int32)
    u = flow_state.reshape(2560, 128)
    xlo, xhi, ylo, yhi, zlo, zhi = call(
        faces_body,
        [((16, 512), F32), ((16, 512), F32), ((320, 128), F32), ((320, 128), F32), ((160, 128), F32), ((160, 128), F32)],
        (u,),
    )
    from_zlo, from_zhi = shifted(zhi, "gz", 1), shifted(zlo, "gz", -1)
    from_ylo, from_yhi = shifted(yhi, "gy", 1), shifted(ylo, "gy", -1)
    from_xlo, from_xhi = shifted(xhi, "gx", 1), shifted(xlo, "gx", -1)
    ax, qx, ay, qy, az, qz, qzy, nx, my, mz = tables(
        idx, advection, inverse_x, inverse_y, inverse_z, reduced_x, reduced_y, reduced_z
    )
    w, bx = call(
        residual_body,
        [((2560, 128), F32), ((24, 512), F32)],
        (u, from_xlo, from_xhi, from_ylo, from_yhi, from_zlo, from_zhi, xlo, xhi, ax, ay, az),
        scratch=[
            ((180, 32, 128), F32),
            ((160, 32, 128), F32),
            ((170, 16, 128), F32),
            ((160, 16, 128), F32),
            ((512, 128), F32),
            ((512, 128), F32),
            ((128, 512), F32),
        ],
    )
    v1, yp, zp = call(
        spread_body,
        [((2560, 128), F32), ((704, 128), F32), ((320, 128), F32)],
        (w, bx, shifted(bx, "gx", 1), shifted(bx, "gx", 2), shifted(bx, "gx", 3), nx, qx),
        scratch=[((128, 512), F32), ((640, 128), F32), ((320, 128), F32)],
    )
    yr, zr = handed(yp, "gy"), handed(zp, "gz")
    yo, st = call(owner_y_body, [((640, 128), F32), ((8, 128), F32)], (yr, my))
    yg = handed(yo, "gy")
    (zo,) = call(owner_z_body, [((384, 128), F32)], (zr, st, mz))
    zg = handed(zo, "gz")
    zc, zy, fin = call(cross_body, [((320, 128), F32), ((640, 128), F32), ((8, 128), F32)], (zg,))
    zyg = handed(zy, "gy")
    (v2,) = call(middle_body, [((2560, 128), F32)], (v1, zc, yg, qz, qy))
    (out,) = call(last_body, [((2560, 128), F32)], (idx, v2, zyg, fin, my, qzy, qy), smem=1)
    return out.reshape(5, 32, 16, 128), fin[0, :VARS]


def solution(mesh):
    spec = P(None, "gz", "gy", "gx")
    return jax.shard_map(
        shards,
        mesh=mesh,
        in_specs=(spec, P(), P(), P(), P(), P(), P(), P()),
        out_specs=(spec, P()),
        check_vma=False,
    )
```

```python
import functools

import jax
import jax.numpy as jnp
from jax import lax
from jax.experimental import pallas as pl
from jax.experimental.pallas import tpu as pltpu
from jax.sharding import PartitionSpec as P

VARS = 5
F32 = jnp.float32
BF16 = jnp.bfloat16
DAMP = 0.0625
COURANT = 8000.0
VMEM = pltpu.VMEM
NN = (((1,), (0,)), ((), ()))
NT = (((1,), (1,)), ((), ()))


def iota(shape, dim):
    return lax.broadcasted_iota(jnp.int32, shape, dim)


def picks(shape, cond):
    return jnp.where(cond(iota(shape, 0), iota(shape, 1)), 1.0, 0.0).astype(BF16)


def split(x):
    hi = x.astype(BF16)
    return hi, (x - hi.astype(F32)).astype(BF16)


def dot1(a, b, dims=NN):
    return lax.dot_general(a, b, dims, preferred_element_type=F32)


def stacked(x):
    hi, lo = split(x)
    return jnp.concatenate([hi, hi, lo], axis=0)


def call(body, out, args, scratch=(), far=(), smem=(), far_out=(), sems=0, flops=1_000_000):
    def spec(k, places):
        if k in smem and places is far:
            return pl.BlockSpec(memory_space=pltpu.SMEM)
        return pl.BlockSpec(memory_space=pl.ANY if k in places else VMEM)

    size = sum(a.size * a.dtype.itemsize for a in args)
    shapes = [VMEM(*t) for t in scratch]
    if sems:
        shapes.append(pltpu.SemaphoreType.DMA((sems,)))
    return pl.pallas_call(
        body,
        out_shape=[jax.ShapeDtypeStruct(*o) for o in out],
        in_specs=[spec(k, far) for k in range(len(args))],
        out_specs=[pl.BlockSpec(memory_space=pl.ANY if k in far_out else VMEM) for k in range(len(out))],
        scratch_shapes=shapes,
        compiler_params=pltpu.CompilerParams(vmem_limit_bytes=24 * 1024 * 1024),
        cost_estimate=pl.CostEstimate(flops=flops, bytes_accessed=size, transcendentals=0),
    )(*args)


def fetch(pairs, sem):
    copies = [pltpu.make_async_copy(a, b, sem.at[k]) for k, (a, b) in enumerate(pairs)]
    for c in copies:
        c.start()
    for c in copies:
        c.wait()


def spread(left, parts, right, keep=None):
    wide = [dot1(dot1(left, part).astype(BF16), right) for part in parts]
    if keep is not None:
        wide = [jnp.where(keep, x, 0.0) for x in wide]
    return [x.astype(BF16) for x in wide]


def masked(shape, cond):
    return cond(iota(shape, 0), iota(shape, 1))


def put(ref, v, halves):
    hi, lo = halves
    k = hi.shape[1]
    ref[v, :, 0:k] = hi
    ref[v, :, k : 2 * k] = lo
    ref[v, :, 2 * k : 3 * k] = hi


def solve_tables_body(invx_far, invy_far, invz_far, ax, ay, az, invx, invy, invz, sem):
    fetch([(invx_far, invx), (invy_far, invy), (invz_far, invz)], sem)

    def per_variable(v, carry):
        hi, lo = split(invx[v].T)
        ax[v, 0:128, :] = hi
        ax[v, 128:256, :] = hi
        ax[v, 256:384, :] = lo
        put(
            ay,
            v,
            spread(
                picks((128, 16), lambda a, k: (a & 15) == k),
                split(invy[v]),
                picks((16, 128), lambda k, c: k == (c & 15)),
                masked((128, 128), lambda a, c: (a >> 4) == (c >> 4)),
            ),
        )
        put(
            az,
            v,
            spread(
                picks((256, 32), lambda a, k: (a >> 3) == k),
                split(invz[v]),
                picks((32, 256), lambda k, c: k == (c >> 3)),
                masked((256, 256), lambda a, c: (a & 7) == (c & 7)),
            ),
        )
        return carry

    lax.fori_loop(0, VARS, per_variable, 0)


def near(red, speed):
    rows = red.shape[0]
    i, k = iota((rows, rows), 0), iota((rows, rows), 1)
    r, d = i & 3, k - (i - (i & 3))
    lower, upper = -0.5 * speed - 2.0, 0.5 * speed - 2.0
    half = jnp.where(
        ((r == 0) & (d == -2)) | ((r == 1) & (d == -1)) | ((r == 2) & (d == 4)) | ((r == 3) & (d == 5)), 0.5, 0.0
    )
    other = jnp.where((r == 0) & (d == -1), lower, jnp.where((r == 3) & (d == 4), upper, 0.0))
    return lax.dot_general(half + other, red, NN, precision=lax.Precision.HIGHEST, preferred_element_type=F32)


def system_tables_body(
    adv, invx_far, redx_far, redy_far, redz_far, nx, qx, my, mz, cy, cz, invx, redx, redy, redz, sem
):
    ix, iy, iz = lax.axis_index("gx"), lax.axis_index("gy"), lax.axis_index("gz")
    fetch([(invx_far, invx), (redx_far, redx), (redy_far, redy), (redz_far, redz)], sem)
    nx[...] = jnp.zeros_like(nx)

    def per_variable(v, carry):
        pick = picks((32, 128), lambda a, c: ((a >> 2) == v) & (c == ((126 + (a & 3)) & 127)))
        hi, lo = [dot1(pick, part, NT).astype(BF16) for part in split(invx[v])]
        qx[v, 0:32, :] = hi
        qx[v, 32:64, :] = hi
        qx[v, 64:96, :] = lo
        parts = split(near(redy[v], adv[1, v]))
        right = picks((32, 128), lambda k, c: k == 4 * (c >> 4) + (c & 3))
        same = masked((128, 128), lambda a, c: ((a >> 2) & 3) == ((c >> 2) & 3))
        put(my, v, spread(picks((128, 32), lambda a, k: k == 4 * (a >> 4) + (a & 3)), parts, right, same))
        same = masked((16, 128), lambda a, c: ((a >> 2) & 3) == ((c >> 2) & 3))
        put(cy, v, spread(picks((16, 32), lambda a, k: k == 4 * iy + (a & 3)), parts, right, same))
        parts = split(near(redz[v], adv[2, v]))
        put(
            mz,
            v,
            spread(
                picks((64, 32), lambda a, k: k == 4 * (a >> 3) + (a & 3)),
                parts,
                picks((32, 64), lambda k, c: k == 4 * (c >> 3) + (c & 3)),
                masked((64, 64), lambda a, c: ((a >> 2) & 1) == ((c >> 2) & 1)),
            ),
        )
        put(
            cz,
            v,
            spread(
                picks((16, 32), lambda a, k: k == 4 * iz + ((a >> 2) & 3)),
                parts,
                picks((32, 128), lambda k, c: k == (c >> 2)),
                masked((16, 128), lambda a, c: (a & 3) == (c & 3)),
            ),
        )
        parts = split(near(redx[v], adv[0, v]))
        left = picks((32, 16), lambda a, k: ((a >> 2) == v) & (k == 4 * ix + ((a & 3) ^ 2)))
        right = picks(
            (16, 128), lambda k, c: (((c >> 2) & 7) == v) & (k == 4 * ((ix + 4 - (c >> 5)) & 3) + ((c & 3) ^ 2))
        )
        hi, lo = spread(left, parts, right)
        nx[:, 0:128] += hi
        nx[:, 128:256] += lo
        nx[:, 256:384] += hi
        return carry

    lax.fori_loop(0, VARS, per_variable, 0)


def column_tables_body(invy_far, invz_far, qy, qz, qzy, invy, invz, sem):
    fetch([(invy_far, invy), (invz_far, invz)], sem)

    def per_variable(v, carry):
        put(
            qy,
            v,
            spread(
                picks((256, 16), lambda a, k: (a & 15) == k),
                split(invy[v]),
                picks((16, 64), lambda k, c: k == (c & 3) + 12 * ((c & 3) >> 1)),
                masked((256, 64), lambda a, c: (((a >> 4) & 7) == (c >> 3)) & ((a >> 7) == ((c >> 2) & 1))),
            ),
        )
        parts = split(invz[v])
        put(
            qz,
            v,
            spread(
                picks((256, 32), lambda a, k: (a >> 3) == k),
                parts,
                picks((32, 32), lambda k, c: k == (c >> 3) + 28 * (c >> 4)),
                masked((256, 32), lambda a, c: (a & 7) == (c & 7)),
            ),
        )
        put(
            qzy,
            v,
            spread(
                picks((128, 32), lambda a, k: k == (2 * (a >> 6) + ((a >> 2) & 1)) * 8 + ((a >> 3) & 7)),
                parts,
                picks((32, 16), lambda k, c: k == (c >> 2) + 28 * (c >> 3)),
                masked((128, 16), lambda a, c: (a & 3) == (c & 3)),
            ),
        )
        return carry

    lax.fori_loop(0, VARS, per_variable, 0)


def faces_body(u, xlo, xhi, ylo, yhi):
    lane = iota((512, 128), 1)
    wide = jnp.zeros((512, 128), F32)
    for v in range(VARS):
        block = u[512 * v : 512 * v + 512, :]
        low = pltpu.roll(block, 2 * v, 1) if v else block
        wide = jnp.where((lane >> 1) == v, low, wide)
        wide = jnp.where((lane >> 1) == 8 + v, pltpu.roll(block, 18 + 2 * v, 1), wide)
        for j in range(2):
            at = 32 * (2 * v + j)
            ylo[at : at + 32, :] = u[pl.ds(512 * v + j, 32, stride=16), :]
            yhi[at : at + 32, :] = u[pl.ds(512 * v + 14 + j, 32, stride=16), :]
    turned = wide.T
    xlo[...] = turned[0:16]
    xhi[...] = turned[16:32]


def primitives(u):
    inverse = 1.0 / u[0]
    velocity = [u[1 + k] * inverse for k in range(3)]
    kinetic = 0.5 * (velocity[0] * velocity[0] + velocity[1] * velocity[1] + velocity[2] * velocity[2])
    internal = jnp.maximum(u[4] * inverse - kinetic, 0.25)
    return velocity, internal, 0.4 * u[0] * internal


def flux(u, velocity, pressure, d):
    w = velocity[d]
    out = [u[1 + d]]
    for k in range(3):
        moment = u[1 + k] * w
        out.append(moment + pressure if k == d else moment)
    out.append((u[4] + pressure) * w)
    return out


def stats_row(shape, sums, top):
    lane = iota(shape, len(shape) - 1)
    row = jnp.where(lane == VARS, top, 0.0)
    for v in range(VARS):
        row = jnp.where(lane == v, sums[v], row)
    return row


def merged_stats(rows):
    lane = iota(rows[0].shape, 1)
    total, top = rows[0], rows[0]
    for row in rows[1:]:
        total, top = total + row, jnp.maximum(top, row)
    return jnp.where(lane < VARS, total, top)


def residual_body(
    u, xlo, xhi, ylo, yhi, zlo, zhi, own_lo, own_hi, ax, ay, az, w, bx, pad, fy, fz, res, fix, half, edge
):
    def fill(z, carry):
        for v in range(VARS):
            pad[36 * v + 2 + z, 8:24, :] = u[pl.ds(pl.multiple_of(512 * v + 16 * z, 16), 16), :]
        return carry

    lax.fori_loop(0, 32, fill, 0)
    rows = pad.reshape(180 * 32, 128)
    for v in range(VARS):
        for k in range(2):
            pad[36 * v + k, 8:24, :] = zlo[32 * v + 16 * k : 32 * v + 16 * k + 16, :]
            pad[36 * v + 34 + k, 8:24, :] = zhi[32 * v + 16 * k : 32 * v + 16 * k + 16, :]
            at = 32 * (2 * v + k)
            rows[pl.ds(32 * (36 * v + 2) + 6 + k, 32, stride=32), :] = ylo[at : at + 32, :]
            rows[pl.ds(32 * (36 * v + 2) + 24 + k, 32, stride=32), :] = yhi[at : at + 32, :]

    edge[...] = jnp.zeros_like(edge)

    def line(ref, j):
        return [ref[2 * v + j : 2 * v + j + 1, :] for v in range(VARS)]

    def fx(u):
        velocity, _, pressure = primitives(u)
        return flux(u, velocity, pressure, 0)

    l2, l1, h1, h2 = line(xlo, 0), line(xlo, 1), line(xhi, 0), line(xhi, 1)
    o0, o1, p1, p0 = line(own_lo, 0), line(own_lo, 1), line(own_hi, 0), line(own_hi, 1)
    fl, fp, fh, fo = fx(l1), fx(p0), fx(h1), fx(o0)
    for v in range(VARS):
        dl, dh = l1[v] - p0[v], h1[v] - o0[v]
        edge[4 * v : 4 * v + 1, :] = -DAMP * dh
        edge[4 * v + 1 : 4 * v + 2, :] = -0.5 * (fh[v] - fo[v]) + 4.0 * DAMP * dh - DAMP * (h2[v] - o1[v])
        edge[4 * v + 2 : 4 * v + 3, :] = 0.5 * (fl[v] - fp[v]) + 4.0 * DAMP * dl - DAMP * (l2[v] - p1[v])
        edge[4 * v + 3 : 4 * v + 4, :] = -DAMP * dl
    fix[...] = edge[...].T

    for z in (-1, 32):
        c = [pad[36 * v + 2 + z, 8:24, :] for v in range(VARS)]
        velocity, _, pressure = primitives(c)
        for v, f in enumerate(flux(c, velocity, pressure, 2)):
            fz[34 * v + 1 + z] = f

    def plane(z, top):
        full = [pad[36 * v + 2 + z] for v in range(VARS)]
        velocity, internal, pressure = primitives(full)
        for v, f in enumerate(flux(full, velocity, pressure, 1)):
            fy[32 * v + z] = f
        c = [f[8:24] for f in full]
        velocity, internal, pressure = [f[8:24] for f in velocity], internal[8:24], pressure[8:24]
        for v, f in enumerate(flux(c, velocity, pressure, 2)):
            fz[34 * v + 1 + z] = f
        for v, f in enumerate(flux(c, velocity, pressure, 0)):
            damped = (4.0 * DAMP) * c[v]
            res[32 * v + z] = (
                pltpu.roll(damped - 0.5 * f, 127, 1)
                + pltpu.roll(damped + 0.5 * f, 1, 1)
                - DAMP * (pltpu.roll(c[v], 126, 1) + pltpu.roll(c[v], 2, 1))
                - (18.0 * DAMP) * c[v]
            )
        speed = jnp.abs(velocity[0]) + jnp.abs(velocity[1]) + jnp.abs(velocity[2])
        return jnp.maximum(top, speed + jnp.sqrt((3.0 * 1.4 * 0.4) * internal))

    top = lax.fori_loop(0, 32, plane, jnp.zeros((16, 128), F32), unroll=2)

    lane = iota((16, 128), 1)
    edges = (lane < 2) | (lane >= 126)

    def finish(z, sums):
        out = []
        fixes = fix[pl.ds(pl.multiple_of(16 * z, 16), 16), :]
        for v in range(VARS):
            at = 36 * v + 2 + z
            ones = (pad[at, 7:23, :] + pad[at, 9:25, :]) + (pad[at - 1, 8:24, :] + pad[at + 1, 8:24, :])
            twos = (pad[at, 6:22, :] + pad[at, 10:26, :]) + (pad[at - 2, 8:24, :] + pad[at + 2, 8:24, :])
            steep = (fy[32 * v + z, 7:23, :] - fy[32 * v + z, 9:25, :]) + (fz[34 * v + z] - fz[34 * v + 2 + z])
            value = res[32 * v + z] + 0.5 * steep + (4.0 * DAMP) * ones - DAMP * twos
            value = value + jnp.where(edges, pltpu.roll(fixes, (126 - 4 * v) & 127, 1), 0.0)
            res[32 * v + z] = value
            out.append(sums[v] + value * value)
        return tuple(out)

    sums = lax.fori_loop(0, 32, finish, tuple(jnp.zeros((16, 128), F32) for _ in range(VARS)), unroll=2)

    def solve(v, carry):
        hi, lo = split(res[pl.ds(32 * v, 32)].reshape(512, 128))
        half[...] = dot1(jnp.concatenate([hi, lo, hi], axis=1), ax[v])
        for g in range(4):
            half[128 * g : 128 * g + 128, :] = dot1(ay[v], stacked(half[128 * g : 128 * g + 128, :]))
        field = half[...].reshape(32, 2, 8, 128)
        parts = [dot1(az[v], stacked(field[:, h].reshape(256, 128))).reshape(32, 1, 8, 128) for h in range(2)]
        w[pl.ds(pl.multiple_of(512 * v, 512), 512), :] = jnp.concatenate(parts, axis=1).reshape(512, 128)
        return carry

    lax.fori_loop(0, VARS, solve, 0)
    lane = iota((512, 128), 1)
    wide = jnp.zeros((512, 128), F32)
    for v in range(VARS):
        wide = jnp.where((lane >> 2) == v, pltpu.roll(w[512 * v : 512 * v + 512, :], 2 + 4 * v, 1), wide)
    turned = wide.T
    bx[...] = turned[0:24]
    bx[20:21, :] = stats_row((1, 512), [jnp.sum(s) for s in sums], jnp.max(top))


def spread_body(w, b0, b1, b2, b3, nx, qx, v1_far, zp, *rest):
    yp, (v1, wide, yb, zb, sem) = rest[:8], rest[8:]
    me = lax.axis_index("gy")
    blank = jnp.zeros((8, 512), F32)
    pieces = [b0, b1, b2, b3]
    data = jnp.concatenate([t for p in pieces for t in (p[...], blank)], axis=0)
    wide[...] = jnp.zeros_like(wide)
    wide[0:32, :] = dot1(nx[...], stacked(data))
    hi, lo = split(wide[...].T[:, 0:32])
    turned = jnp.concatenate([hi, lo, hi], axis=1)

    def out_copy(v):
        at = pl.ds(pl.multiple_of(512 * v, 512), 512)
        return pltpu.make_async_copy(v1.at[at], v1_far.at[at], sem.at[v])

    def correct(v, carry):
        at = pl.ds(pl.multiple_of(512 * v, 512), 512)
        v1[at, :] = w[at, :] - dot1(turned, qx[v])
        out_copy(v).start()
        return carry

    lax.fori_loop(0, VARS, correct, 0)
    for v in range(VARS):
        for h in range(2):
            for j, z in enumerate((0, 1, 30, 31)):
                at = ((v * 2 + h) * 4 + j) * 8
                zb[at : at + 8, :] = v1[512 * v + 16 * z + 8 * h : 512 * v + 16 * z + 8 * h + 8, :]
    for p in range(8):
        zp[40 * p : 40 * p + 40, :] = zb[pl.ds(p, 40, stride=8), :]
    for v in range(VARS):
        for j, y in enumerate((0, 1, 14, 15)):
            for t in range(4):
                at = ((v * 4 + t) * 4 + j) * 8
                yb[at : at + 8, :] = v1[pl.ds(512 * v + 128 * t + y, 8, stride=16), :]
            for k, z in enumerate((0, 30)):
                lines = v1[pl.ds(512 * v + 16 * z + y, 2, stride=16), :]
                yp[0][pl.ds(80 + 16 * v + 8 * k + j, 2, stride=4), :] = lines
    stats = merged_stats([p[20:21, 0:128] for p in pieces])
    yp[0][160:168, :] = jnp.broadcast_to(stats, (8, 128))
    shared = yp[0][80:168, :]
    for k in range(8):
        yp[k][0:80, :] = yb[pl.ds(me ^ k, 80, stride=8), :]
        if k:
            yp[k][80:168, :] = shared
    for v in range(VARS):
        out_copy(v).wait()


def owner_y_body(*refs):
    yr, (my, cy), yo, (cross, st, data, more, solved) = refs[:8], refs[8:10], refs[10:18], refs[18:]
    me = lax.axis_index("gy")
    for k in range(8):
        for v in range(VARS):
            at = pl.ds(pl.multiple_of(128 * v + 16 * (me ^ k), 16), 16)
            data[at, :] = yr[k][16 * v : 16 * v + 16, :]
            more[at, :] = yr[k][80 + 16 * v : 96 + 16 * v, :]

    def one(v, carry):
        rows = pl.ds(pl.multiple_of(128 * v, 128), 128)
        solved[rows, :] = dot1(my[v], stacked(data[rows, :]))
        cross[pl.ds(pl.multiple_of(16 * v, 16), 16), :] = dot1(cy[v], stacked(more[rows, :]))
        return carry

    lax.fori_loop(0, VARS, one, 0)
    for k in range(8):
        for v in range(VARS):
            at = pl.ds(pl.multiple_of(128 * v + 16 * (me ^ k), 16), 16)
            yo[k][16 * v : 16 * v + 16, :] = solved[at, :]
    st[...] = merged_stats([r[160:168, :] for r in yr])


def owner_z_body(zr, cross, st, mz, zo):
    def one(v, carry):
        at = pl.multiple_of(8 * v, 8)
        data = jnp.concatenate([zr[pl.ds(40 * q + at, 8), :] for q in range(8)], axis=0)
        out = dot1(mz[v], stacked(data))
        for p in range(8):
            zo[pl.ds(128 * p + at, 8), :] = out[8 * p : 8 * p + 8]
        return carry

    lax.fori_loop(0, VARS, one, 0)
    for p in range(8):
        zo[128 * p + 40 : 128 * p + 120, :] = cross[...]
        zo[128 * p + 120 : 128 * p + 128, :] = st[...]


def middle_body(v1_far, *refs):
    yg, qy, v2, v1, data, sem = refs[:8], refs[8], refs[9], refs[10], refs[11], refs[12]
    me = lax.axis_index("gy")

    def in_copy(v):
        at = pl.ds(pl.multiple_of(512 * v, 512), 512)
        return pltpu.make_async_copy(v1_far.at[at], v1.at[at], sem.at[v])

    for v in range(VARS):
        in_copy(v).start()
    for k in range(8):
        for t in range(2 * VARS):
            data[pl.ds(pl.multiple_of(64 * t + 8 * (me ^ k), 8), 8), :] = yg[k][8 * t : 8 * t + 8, :]

    def one(v, carry):
        in_copy(v).wait()
        for t in range(2):
            at = pl.ds(pl.multiple_of(512 * v + 256 * t, 256), 256)
            lines = data[pl.ds(pl.multiple_of(128 * v + 64 * t, 64), 64), :]
            v2[at, :] = v1[at, :] - dot1(qy[v], stacked(lines))
        return carry

    lax.fori_loop(0, VARS, one, 0)


def last_body(v2, zg, cz, qz, qzy, qy, out_far, fin, out, zc, sem):
    for v in range(VARS):
        for h in range(2):
            for r in range(4):
                at = ((v * 2 + h) * 4 + r) * 8
                zc[at : at + 8, :] = zg[pl.ds(8 * v + 4 * h + r, 8, stride=128), :]
    stats = merged_stats([zg[128 * q + 120 : 128 * q + 128, :] for q in range(8)])
    lane = iota((8, 128), 1)
    step = COURANT / jnp.max(jnp.where(lane == VARS, stats, 0.0))
    fin[...] = jnp.sqrt(stats * (1.0 / 16777216.0))

    def out_copy(v):
        at = pl.ds(pl.multiple_of(512 * v, 512), 512)
        return pltpu.make_async_copy(out.at[at], out_far.at[at], sem.at[v])

    def one(v, carry):
        at = pl.multiple_of(40 + 16 * v, 8)
        data = jnp.concatenate([zg[pl.ds(128 * q + at, 16), :] for q in range(8)], axis=0)
        lines = dot1(qzy[v], stacked(dot1(cz[v], stacked(data))))
        parts = []
        for h in range(2):
            rows = zc[pl.ds(pl.multiple_of(64 * v + 32 * h, 32), 32), :]
            parts.append(dot1(qz[v], stacked(rows)).reshape(32, 1, 8, 128))
        planes = jnp.concatenate(parts, axis=1).reshape(512, 128)
        for t in range(2):
            at = pl.ds(pl.multiple_of(512 * v + 256 * t, 256), 256)
            back = dot1(qy[v], stacked(lines[64 * t : 64 * t + 64]))
            out[at, :] = step * (v2[at, :] - planes[256 * t : 256 * t + 256] + back)
        out_copy(v).start()
        return carry

    lax.fori_loop(0, VARS, one, 0)
    for v in range(VARS):
        out_copy(v).wait()


def handed(x, axis):
    return lax.all_to_all(x, axis, 0, 0, tiled=True)


def shifted(x, axis, by):
    size = lax.axis_size(axis)
    return lax.ppermute(x, axis, [(i, (i + by) % size) for i in range(size)])


def swapped(x, axis, k):
    return lax.ppermute(x, axis, [(i, i ^ k) for i in range(lax.axis_size(axis))])


def shards(flow_state, advection, inverse_x, inverse_y, inverse_z, reduced_x, reduced_y, reduced_z):
    u = flow_state.reshape(2560, 128)
    zlo = flow_state[:, 0:2].reshape(160, 128)
    zhi = flow_state[:, 30:32].reshape(160, 128)
    from_zlo, from_zhi = shifted(zhi, "gz", 1), shifted(zlo, "gz", -1)
    xlo, xhi, ylo, yhi = call(
        faces_body, [((16, 512), F32), ((16, 512), F32), ((320, 128), F32), ((320, 128), F32)], (u,)
    )
    from_ylo, from_yhi = shifted(yhi, "gy", 1), shifted(ylo, "gy", -1)
    from_xlo, from_xhi = shifted(xhi, "gx", 1), shifted(xlo, "gx", -1)
    ax, ay, az = call(
        solve_tables_body,
        [((5, 384, 128), BF16), ((5, 128, 384), BF16), ((5, 256, 768), BF16)],
        (inverse_x, inverse_y, inverse_z),
        scratch=[((5, 128, 128), F32), ((5, 16, 16), F32), ((5, 32, 32), F32)],
        far=(0, 1, 2),
        sems=3,
    )
    w, bx = call(
        residual_body,
        [((2560, 128), F32), ((24, 512), F32)],
        (u, from_xlo, from_xhi, from_ylo, from_yhi, from_zlo, from_zhi, xlo, xhi, ax, ay, az),
        scratch=[
            ((180, 32, 128), F32),
            ((160, 32, 128), F32),
            ((170, 16, 128), F32),
            ((160, 16, 128), F32),
            ((512, 128), F32),
            ((512, 128), F32),
            ((128, 512), F32),
        ],
    )
    pieces = [bx] + [shifted(bx, "gx", k) for k in (1, 2, 3)]
    nx, qx, my, mz, cy, cz = call(
        system_tables_body,
        [
            ((32, 384), BF16),
            ((5, 96, 128), BF16),
            ((5, 128, 384), BF16),
            ((5, 64, 192), BF16),
            ((5, 16, 384), BF16),
            ((5, 16, 384), BF16),
        ],
        (advection, inverse_x, reduced_x, reduced_y, reduced_z),
        scratch=[((5, 128, 128), F32), ((5, 16, 16), F32), ((5, 32, 32), F32), ((5, 32, 32), F32)],
        smem=(0,),
        far=(1, 2, 3, 4),
        sems=4,
    )
    v1, zp, *yp = call(
        spread_body,
        [((2560, 128), F32), ((320, 128), F32)] + [((168, 128), F32)] * 8,
        (w, *pieces, nx, qx),
        scratch=[((2560, 128), F32), ((128, 512), F32), ((640, 128), F32), ((320, 128), F32)],
        far_out=(0,),
        sems=5,
    )
    zr = handed(zp, "gz")
    yr = [yp[0]] + [swapped(yp[k], "gy", k) for k in range(1, 8)]
    *yo, cross, st = call(
        owner_y_body,
        [((80, 128), F32)] * 9 + [((8, 128), F32)],
        (*yr, my, cy),
        scratch=[((640, 128), F32)] * 3,
    )
    (zo,) = call(owner_z_body, [((1024, 128), F32)], (zr, cross, st, mz))
    zg = handed(zo, "gz")
    yg = [yo[0]] + [swapped(yo[k], "gy", k) for k in range(1, 8)]
    qy, qz, qzy = call(
        column_tables_body,
        [((5, 256, 192), BF16), ((5, 256, 96), BF16), ((5, 128, 48), BF16)],
        (inverse_y, inverse_z),
        scratch=[((5, 16, 16), F32), ((5, 32, 32), F32)],
        far=(0, 1),
        sems=2,
    )
    (v2,) = call(
        middle_body,
        [((2560, 128), F32)],
        (v1, *yg, qy),
        scratch=[((2560, 128), F32), ((640, 128), F32)],
        far=(0,),
        sems=5,
    )
    out, fin = call(
        last_body,
        [((2560, 128), F32), ((8, 128), F32)],
        (v2, zg, cz, qz, qzy, qy),
        scratch=[((2560, 128), F32), ((320, 128), F32)],
        far_out=(0,),
        sems=5,
    )
    return out.reshape(5, 32, 16, 128), fin[0, :VARS]


def solution(mesh):
    spec = P(None, "gz", "gy", "gx")
    return jax.shard_map(
        shards,
        mesh=mesh,
        in_specs=(spec, P(), P(), P(), P(), P(), P(), P()),
        out_specs=(spec, P()),
        check_vma=False,
    )
```

```python
import functools

import jax
import jax.numpy as jnp
from jax import lax
from jax.experimental import pallas as pl
from jax.experimental.pallas import tpu as pltpu
from jax.sharding import PartitionSpec as P

VARS = 5
F32 = jnp.float32
BF16 = jnp.bfloat16
DAMP = 0.0625
COURANT = 8000.0
VMEM = pltpu.VMEM
NN = (((1,), (0,)), ((), ()))
NT = (((1,), (1,)), ((), ()))


def iota(shape, dim):
    return lax.broadcasted_iota(jnp.int32, shape, dim)


def picks(shape, cond):
    return jnp.where(cond(iota(shape, 0), iota(shape, 1)), 1.0, 0.0).astype(BF16)


def split(x):
    hi = x.astype(BF16)
    return hi, (x - hi.astype(F32)).astype(BF16)


def dot1(a, b, dims=NN):
    return lax.dot_general(a, b, dims, preferred_element_type=F32)


def stacked(x):
    hi, lo = split(x)
    return jnp.concatenate([hi, hi, lo], axis=0)


def small_solve(table, pieces):
    return dot1(table, stacked(jnp.concatenate(pieces, axis=0)))


def call(body, out, args, scratch=(), far=(), smem=(), far_out=(), smem_out=(), sems=0, limit=24, flops=1_000_000):
    def spec(k, places):
        if k in smem and places is far:
            return pl.BlockSpec(memory_space=pltpu.SMEM)
        return pl.BlockSpec(memory_space=pltpu.HBM if k in places else VMEM)

    size = sum(a.size * a.dtype.itemsize for a in args)
    shapes = [VMEM(*t) for t in scratch]
    if sems:
        shapes.append(pltpu.SemaphoreType.DMA((sems,)))
    return pl.pallas_call(
        body,
        out_shape=[jax.ShapeDtypeStruct(*o) for o in out],
        in_specs=[spec(k, far) for k in range(len(args))],
        out_specs=[
            pl.BlockSpec(memory_space=pltpu.SMEM if k in smem_out else pltpu.HBM if k in far_out else VMEM)
            for k in range(len(out))
        ],
        scratch_shapes=shapes,
        compiler_params=pltpu.CompilerParams(vmem_limit_bytes=limit * 1024 * 1024),
        cost_estimate=pl.CostEstimate(flops=flops, bytes_accessed=size, transcendentals=0),
    )(*args)


def fetch(pairs, sem):
    copies = [pltpu.make_async_copy(a, b, sem.at[k]) for k, (a, b) in enumerate(pairs)]
    for c in copies:
        c.start()
    for c in copies:
        c.wait()


def spread(left, parts, right, keep=None):
    wide = [dot1(dot1(left, part).astype(BF16), right) for part in parts]
    if keep is not None:
        wide = [jnp.where(keep, x, 0.0) for x in wide]
    return [x.astype(BF16) for x in wide]


def masked(shape, cond):
    return cond(iota(shape, 0), iota(shape, 1))


def put(ref, v, halves):
    hi, lo = halves
    k = hi.shape[1]
    ref[v, :, 0:k] = hi
    ref[v, :, k : 2 * k] = lo
    ref[v, :, 2 * k : 3 * k] = hi


def solve_tables_body(invx, invy, invz, ax, ay, az, qx):
    y_left = picks((128, 16), lambda a, k: (a & 15) == k)
    y_right = picks((16, 128), lambda k, c: k == (c & 15))
    y_same = masked((128, 128), lambda a, c: (a >> 4) == (c >> 4))
    z_left = picks((256, 32), lambda a, k: (a >> 3) == k)
    z_right = picks((32, 256), lambda k, c: k == (c >> 3))
    z_same = masked((256, 256), lambda a, c: (a & 7) == (c & 7))
    qx[...] = jnp.zeros_like(qx)
    for v in range(VARS):
        turned = invx[v].T
        qx[4 * v : 4 * v + 2, :] = turned[126:128]
        qx[4 * v + 2 : 4 * v + 4, :] = turned[0:2]
        hi, lo = split(turned)
        ax[v, 0:128, :] = hi
        ax[v, 128:256, :] = hi
        ax[v, 256:384, :] = lo
        put(ay, v, spread(y_left, split(invy[v]), y_right, y_same))
        put(az, v, spread(z_left, split(invz[v]), z_right, z_same))


def first_off(r):
    return r - 2 + 4 * (r >> 1)


def second_off(r):
    return jnp.where(r == 0, -1, jnp.where(r == 3, 4, -4096))


def near(chosen, red, row, speed):
    hi, lo = split(red)
    both = dot1(chosen, hi) + dot1(chosen, lo)
    rows = both.shape[0] // 2
    other = jnp.where(row == 0, -0.5 * speed - 2.0, jnp.where(row == 3, 0.5 * speed - 2.0, 0.0))
    return 0.5 * both[0:rows] + other * both[rows:]


def exact(a, b):
    return lax.dot_general(a, b, NN, precision=lax.Precision.HIGHEST, preferred_element_type=F32)


def z_tables(adv, redz, tz, mz):
    iz = lax.axis_index("gz")
    row, lane = iota((32, 32), 0), iota((32, 32), 1)
    block, first = lane >> 2, row - (lane - (lane & 3))
    start = jnp.where(block < iz, 2, 0)
    here = block[0:8] == iz
    low = (iota((8, 32), 0) & 3) < 2
    chosen = jnp.concatenate(
        [picks((8, 32), lambda a, k, f=f: k == 4 * iz + f(a & 3)) for f in (first_off, second_off)], axis=0
    )
    same = jnp.where((row >> 2) == block, 1.0, 0.0)
    gather = jnp.where(
        iota((128, 32), 1)
        == jnp.where(
            iota((128, 32), 0) < 64,
            2 * ((iota((128, 32), 0) & 31) >> 2) + (iota((128, 32), 0) >> 5),
            14 + (iota((128, 32), 0) >> 5),
        ),
        1.0,
        0.0,
    )
    send_left = picks((32, 32), lambda a, k: k == 4 * iz + (a >> 3))
    send_right = picks((32, 32), lambda k, c: k == 4 * iz + (c >> 3))
    send_same = masked((32, 32), lambda a, c: (a & 7) == (c & 7))
    left = picks((32, 8), lambda a, k: k == (a >> 3))
    right = picks((32, 144), lambda k, c: k == (c >> 3))
    keep = masked((32, 144), lambda a, c: (a & 7) == (c & 7))
    for v in range(VARS):
        put(tz, v, spread(send_left, split(redz[v]), send_right, send_same))
        red = redz[v]

        def line(which):
            return jnp.sum(jnp.where(which, red, 0.0), axis=0, keepdims=True)

        a0, a1 = line(first == start), line(first == start + 1)
        e0, e1 = line(first == 2), line(first == 3)
        blank = jnp.zeros((2, 32), F32)
        sums = exact(jnp.concatenate([a0 * a0, a0 * a1, a1 * a1, e0 * e0, e0 * e1, e1 * e1, blank], axis=0), same)

        def dual(u0, u1, g):
            scale = 1.0 / (g[0:1] * g[2:3] - g[1:2] * g[1:2])
            return (g[2:3] * u0 - g[1:2] * u1) * scale, (g[0:1] * u1 - g[1:2] * u0) * scale

        p0, p1 = dual(a0, a1, sums[0:3])
        f0, f1 = dual(e0, e1, sums[3:6])
        needed = near(chosen, red, iota((8, 32), 0) & 3, adv[2, v])
        sent = jnp.where(here & ~low, 0.0, needed)
        own = jnp.where(here & ~low, needed, 0.0)
        table = exact(jnp.concatenate([sent * p0, sent * p1, own * f0, own * f1], axis=1), gather)
        put(mz, v, spread(left, split(table), right, keep))


def system_tables_body(adv, redx, redy, redz, nx, ny, tz, mz):
    ix, iy = lax.axis_index("gx"), lax.axis_index("gy")

    def choose(at):
        return jnp.concatenate(
            [picks((32, 32), lambda a, k, f=f: k == at(a >> 2) * 4 + f(a & 3)) for f in (first_off, second_off)], axis=0
        )

    def tripled(at):
        def pick(which):
            return picks((32, 96), lambda k, c: (((c >> 5) == 1) == which) & (k == 4 * at((c >> 2) & 7) + (c & 3)))

        return pick(False), pick(True)

    row = iota((32, 32), 0) & 3
    chosen = choose(lambda k: iy ^ k)
    ends, inner = tripled(lambda k: iy ^ k)
    for v in range(VARS):
        hi, lo = split(near(chosen, redy[v], row, adv[1, v]))
        ny[v] = (dot1(hi, ends) + dot1(lo, inner)).astype(BF16)
    z_tables(adv, redz, tz, mz)
    total = None
    row = (iota((32, 16), 0) & 3) ^ 2
    for v in range(VARS):
        chosen = jnp.concatenate(
            [
                picks((32, 16), lambda a, k, f=f: ((a >> 2) == v) & (k == 4 * ix + f((a & 3) ^ 2)))
                for f in (first_off, second_off)
            ],
            axis=0,
        )
        term = near(chosen, redx[v], row, adv[0, v])
        total = term if total is None else total + term
    right = picks((16, 128), lambda k, c: k == 4 * ((ix + 4 - (c >> 5)) & 3) + ((c & 3) ^ 2))
    same = masked((32, 128), lambda a, c: (a >> 2) == ((c >> 2) & 7))
    hi, lo = [jnp.where(same, dot1(part, right), 0.0).astype(BF16) for part in split(total)]
    nx[:, 0:128] = hi
    nx[:, 128:256] = lo
    nx[:, 256:384] = hi


def column_tables_body(invy_far, invz_far, qy, qz, qzy, invy, invz, sem):
    fetch([(invy_far, invy), (invz_far, invz)], sem)

    for v in range(VARS):
        put(
            qy,
            v,
            spread(
                picks((256, 16), lambda a, k: (a & 15) == k),
                split(invy[v]),
                picks((16, 64), lambda k, c: k == (c & 3) + 12 * ((c & 3) >> 1)),
                masked((256, 64), lambda a, c: (((a >> 4) & 7) == (c >> 3)) & ((a >> 7) == ((c >> 2) & 1))),
            ),
        )
        parts = split(invz[v])
        put(
            qz,
            v,
            spread(
                picks((256, 32), lambda a, k: (a >> 3) == k),
                parts,
                picks((32, 32), lambda k, c: k == (c >> 3) + 28 * (c >> 4)),
                masked((256, 32), lambda a, c: (a & 7) == (c & 7)),
            ),
        )
        put(
            qzy,
            v,
            spread(
                picks((128, 32), lambda a, k: k == (2 * (a >> 6) + ((a >> 2) & 1)) * 8 + ((a >> 3) & 7)),
                parts,
                picks((32, 16), lambda k, c: k == (c >> 2) + 28 * (c >> 3)),
                masked((128, 16), lambda a, c: (a & 3) == (c & 3)),
            ),
        )


def faces_body(u, invx, invy, invz, xlo, xhi, ylo, yhi, zlo, zhi, keptx, kepty, keptz):
    lane = iota((512, 128), 1)
    wide = jnp.zeros((512, 128), F32)
    for v in range(VARS):
        block = u[512 * v : 512 * v + 512, :]
        low = pltpu.roll(block, 2 * v, 1) if v else block
        wide = jnp.where((lane >> 1) == v, low, wide)
        wide = jnp.where((lane >> 1) == 8 + v, pltpu.roll(block, 18 + 2 * v, 1), wide)
        for j in range(2):
            at = 32 * (2 * v + j)
            ylo[at : at + 32, :] = u[pl.ds(512 * v + j, 32, stride=16), :]
            yhi[at : at + 32, :] = u[pl.ds(512 * v + 14 + j, 32, stride=16), :]
        zlo[32 * v : 32 * v + 32, :] = u[512 * v : 512 * v + 32, :]
        zhi[32 * v : 32 * v + 32, :] = u[512 * v + 480 : 512 * v + 512, :]
    turned = wide.T
    xlo[...] = turned[0:16]
    xhi[...] = turned[16:32]
    keptx[...] = invx[...]
    kepty[...] = invy[...]
    keptz[...] = invz[...]


def primitives(u):
    inverse = 1.0 / u[0]
    velocity = [u[1 + k] * inverse for k in range(3)]
    kinetic = 0.5 * (velocity[0] * velocity[0] + velocity[1] * velocity[1] + velocity[2] * velocity[2])
    internal = jnp.maximum(u[4] * inverse - kinetic, 0.25)
    return velocity, internal, 0.4 * u[0] * internal


def flux(u, velocity, pressure, d):
    w = velocity[d]
    out = [u[1 + d]]
    for k in range(3):
        moment = u[1 + k] * w
        out.append(moment + pressure if k == d else moment)
    out.append((u[4] + pressure) * w)
    return out


def stats_row(shape, sums, top):
    lane = iota(shape, len(shape) - 1)
    row = jnp.where(lane == VARS, top, 0.0)
    for v in range(VARS):
        row = jnp.where(lane == v, sums[v], row)
    return row


def merged_stats(rows):
    lane = iota(rows[0].shape, 1)
    total, top = rows[0], rows[0]
    for row in rows[1:]:
        total, top = total + row, jnp.maximum(top, row)
    return jnp.where(lane < VARS, total, top)


def residual_body(
    u, xlo, xhi, ylo, yhi, zlo, zhi, own_lo, own_hi, ax, ay, az, w, bx, pad, fy, fz, res, fix, half, edge
):
    def fill(z, carry):
        for v in range(VARS):
            pad[36 * v + 2 + z, 8:24, :] = u[pl.ds(pl.multiple_of(512 * v + 16 * z, 16), 16), :]
        return carry

    lax.fori_loop(0, 32, fill, 0)
    rows = pad.reshape(180 * 32, 128)
    for v in range(VARS):
        for k in range(2):
            pad[36 * v + k, 8:24, :] = zlo[32 * v + 16 * k : 32 * v + 16 * k + 16, :]
            pad[36 * v + 34 + k, 8:24, :] = zhi[32 * v + 16 * k : 32 * v + 16 * k + 16, :]
            at = 32 * (2 * v + k)
            rows[pl.ds(32 * (36 * v + 2) + 6 + k, 32, stride=32), :] = ylo[at : at + 32, :]
            rows[pl.ds(32 * (36 * v + 2) + 24 + k, 32, stride=32), :] = yhi[at : at + 32, :]

    edge[...] = jnp.zeros_like(edge)

    def line(ref, j):
        return [ref[2 * v + j : 2 * v + j + 1, :] for v in range(VARS)]

    def fx(u):
        velocity, _, pressure = primitives(u)
        return flux(u, velocity, pressure, 0)

    l2, l1, h1, h2 = line(xlo, 0), line(xlo, 1), line(xhi, 0), line(xhi, 1)
    o0, o1, p1, p0 = line(own_lo, 0), line(own_lo, 1), line(own_hi, 0), line(own_hi, 1)
    fl, fp, fh, fo = fx(l1), fx(p0), fx(h1), fx(o0)
    for v in range(VARS):
        dl, dh = l1[v] - p0[v], h1[v] - o0[v]
        edge[4 * v : 4 * v + 1, :] = -DAMP * dh
        edge[4 * v + 1 : 4 * v + 2, :] = -0.5 * (fh[v] - fo[v]) + 4.0 * DAMP * dh - DAMP * (h2[v] - o1[v])
        edge[4 * v + 2 : 4 * v + 3, :] = 0.5 * (fl[v] - fp[v]) + 4.0 * DAMP * dl - DAMP * (l2[v] - p1[v])
        edge[4 * v + 3 : 4 * v + 4, :] = -DAMP * dl
    fix[...] = edge[...].T

    for z in (-1, 32):
        c = [pad[36 * v + 2 + z, 8:24, :] for v in range(VARS)]
        velocity, _, pressure = primitives(c)
        for v, f in enumerate(flux(c, velocity, pressure, 2)):
            fz[34 * v + 1 + z] = f

    def plane(z, top):
        full = [pad[36 * v + 2 + z] for v in range(VARS)]
        velocity, internal, pressure = primitives(full)
        for v, f in enumerate(flux(full, velocity, pressure, 1)):
            fy[32 * v + z] = f
        c = [f[8:24] for f in full]
        velocity, internal, pressure = [f[8:24] for f in velocity], internal[8:24], pressure[8:24]
        for v, f in enumerate(flux(c, velocity, pressure, 2)):
            fz[34 * v + 1 + z] = f
        for v, f in enumerate(flux(c, velocity, pressure, 0)):
            damped = (4.0 * DAMP) * c[v]
            res[32 * v + z] = (
                pltpu.roll(damped - 0.5 * f, 127, 1)
                + pltpu.roll(damped + 0.5 * f, 1, 1)
                - DAMP * (pltpu.roll(c[v], 126, 1) + pltpu.roll(c[v], 2, 1))
                - (18.0 * DAMP) * c[v]
            )
        speed = jnp.abs(velocity[0]) + jnp.abs(velocity[1]) + jnp.abs(velocity[2])
        return jnp.maximum(top, speed + jnp.sqrt((3.0 * 1.4 * 0.4) * internal))

    top = lax.fori_loop(0, 32, plane, jnp.zeros((16, 128), F32), unroll=2)

    lane = iota((16, 128), 1)
    edges = (lane < 2) | (lane >= 126)

    def finish(z, sums):
        out = []
        fixes = fix[pl.ds(pl.multiple_of(16 * z, 16), 16), :]
        for v in range(VARS):
            at = 36 * v + 2 + z
            ones = (pad[at, 7:23, :] + pad[at, 9:25, :]) + (pad[at - 1, 8:24, :] + pad[at + 1, 8:24, :])
            twos = (pad[at, 6:22, :] + pad[at, 10:26, :]) + (pad[at - 2, 8:24, :] + pad[at + 2, 8:24, :])
            steep = (fy[32 * v + z, 7:23, :] - fy[32 * v + z, 9:25, :]) + (fz[34 * v + z] - fz[34 * v + 2 + z])
            value = res[32 * v + z] + 0.5 * steep + (4.0 * DAMP) * ones - DAMP * twos
            value = value + jnp.where(edges, pltpu.roll(fixes, (126 - 4 * v) & 127, 1), 0.0)
            res[32 * v + z] = value
            out.append(sums[v] + value * value)
        return tuple(out)

    sums = lax.fori_loop(0, 32, finish, tuple(jnp.zeros((16, 128), F32) for _ in range(VARS)), unroll=2)

    for v in range(VARS):
        hi, lo = split(res[pl.ds(32 * v, 32)].reshape(512, 128))
        half[...] = dot1(jnp.concatenate([hi, lo, hi], axis=1), ax[v])
        for g in range(4):
            half[128 * g : 128 * g + 128, :] = dot1(ay[v], stacked(half[128 * g : 128 * g + 128, :]))
        field = half[...].reshape(32, 2, 8, 128)
        parts = [dot1(az[v], stacked(field[:, h].reshape(256, 128))).reshape(32, 1, 8, 128) for h in range(2)]
        w[pl.ds(pl.multiple_of(512 * v, 512), 512), :] = jnp.concatenate(parts, axis=1).reshape(512, 128)
    lane = iota((512, 128), 1)
    wide = jnp.zeros((512, 128), F32)
    for v in range(VARS):
        wide = jnp.where((lane >> 2) == v, pltpu.roll(w[512 * v : 512 * v + 512, :], 2 + 4 * v, 1), wide)
    turned = wide.T
    bx[...] = turned[0:24]
    bx[20:21, :] = stats_row((1, 512), [jnp.sum(s) for s in sums], jnp.max(top))


def spread_body(w, b0, b1, b2, b3, nx, qx, tz, v1_far, zp, mine, *rest):
    own, give, (v1, wide, yb, sem) = rest[:4], rest[4], rest[5:]
    me, iz = lax.axis_index("gy"), lax.axis_index("gz")
    blank = jnp.zeros((8, 512), F32)
    pieces = [b0, b1, b2, b3]
    data = jnp.concatenate([t for p in pieces for t in (p[...], blank)], axis=0)
    wide[...] = jnp.zeros_like(wide)
    wide[0:32, :] = dot1(nx[...], stacked(data))
    hi, lo = split(wide[...].T[:, 0:32])
    turned = jnp.concatenate([hi, lo, hi], axis=1)
    copies = []
    for v in range(VARS):
        at = pl.ds(512 * v, 512)
        hi, lo = split(jnp.where((iota((32, 128), 0) >> 2) == v, qx[...], 0.0))
        v1[at, :] = w[at, :] - dot1(turned, jnp.concatenate([hi, hi, lo], axis=0))
        copies.append(pltpu.make_async_copy(v1.at[at], v1_far.at[at], sem.at[v]))
        copies[v].start()
        for h in range(2):
            ends = [v1[512 * v + 16 * z + 8 * h : 512 * v + 16 * z + 8 * h + 8, :] for z in (0, 1, 30, 31)]
            sent = small_solve(tz[v], ends)
            at = 16 * (2 * v + h)
            mine[at : at + 16, :] = sent[16:32]
            for p in range(8):
                zp[168 * p + at : 168 * p + at + 16, :] = jnp.where(p <= iz, sent[0:16], sent[16:32])
        for j, y in enumerate((0, 1, 14, 15)):
            for t in range(4):
                to = ((v * 4 + t) * 4 + j) * 8
                yb[to : to + 8, :] = v1[pl.ds(512 * v + 128 * t + y, 8, stride=16), :]
    stats = jnp.broadcast_to(merged_stats([p[20:21, 0:128] for p in pieces]), (8, 128))
    for p in range(8):
        zp[168 * p + 160 : 168 * p + 168, :] = stats
        to = give.at[pl.ds(80 * (p >> 1), 80)] if p & 1 else own[p >> 1]
        to[...] = yb[pl.ds(me ^ p, 80, stride=8), :]
    for c in copies:
        c.wait()


def pair_body(*refs):
    own, got, out = refs[:3], refs[3], refs[4:]
    for j in range(3):
        out[j][0:80, :] = own[j][...]
        out[j][80:160, :] = got[80 * (j + 1) : 80 * (j + 2), :]


def exchanged(own, give):
    got = swapped(give, "gy", 1)
    out = call(pair_body, [((160, 128), F32)] * 3, (*own[1:], got))
    return [own[0], got] + [swapped(out[j - 1], "gy", 2 * j) for j in (1, 2, 3)]


def chip_lines(first, got, others):
    return [first, got] + [x.at[pl.ds(80 * h, 80)] for x in others for h in range(2)]


def owners_body(*refs):
    yr, ny, own, give = chip_lines(refs[0], refs[1], refs[2:5]), refs[5], refs[6:10], refs[10]
    yo = [give.at[pl.ds(80 * (k >> 1), 80)] if k & 1 else own[k >> 1] for k in range(8)]
    for v in range(VARS):
        for t in range(4):
            at = 16 * v + 4 * t
            out = small_solve(ny[v], [r[at : at + 4, :] for r in yr])
            for k in range(8):
                yo[k][at : at + 4, :] = out[4 * k : 4 * k + 4]


def cross_body(zr, mine, mz, *refs):
    yg, (zy, zc, data) = chip_lines(refs[0], refs[1], refs[2:5]), refs[5:]
    me = lax.axis_index("gy")
    for v in range(VARS):
        for h in range(2):
            at = 16 * (2 * v + h)
            got = [zr[168 * q + at : 168 * q + at + 16, :] for q in range(8)] + [mine[at : at + 16, :]]
            zc[2 * at : 2 * at + 32, :] = small_solve(mz[v], got)
        for j, (h, y) in enumerate(((0, 0), (0, 1), (1, 6), (1, 7))):
            zy[pl.ds(16 * v + j, 4, stride=4), :] = zc[pl.ds(32 * (2 * v + h) + y, 4, stride=8), :]
        for k in range(8):
            for t in range(2 * v, 2 * v + 2):
                data[pl.ds(pl.multiple_of(64 * t + 8 * (me ^ k), 8), 8), :] = yg[k][8 * t : 8 * t + 8, :]
    zy[80:88, :] = merged_stats([zr[168 * q + 160 : 168 * q + 168, :] for q in range(8)])


def middle_body(v1_far, zc, data, qy, qz, v2, v1, sem):
    copies = [
        pltpu.make_async_copy(v1_far.at[pl.ds(512 * v, 512)], v1.at[pl.ds(512 * v, 512)], sem.at[v])
        for v in range(VARS)
    ]
    for c in copies:
        c.start()
    for v in range(VARS):
        parts = []
        for h in range(2):
            rows = zc[64 * v + 32 * h : 64 * v + 32 * h + 32, :]
            parts.append(dot1(qz[v], stacked(rows)).reshape(32, 1, 8, 128))
        planes = jnp.concatenate(parts, axis=1).reshape(512, 128)
        copies[v].wait()
        for t in range(2):
            at = pl.ds(512 * v + 256 * t, 256)
            lines = dot1(qy[v], stacked(data[128 * v + 64 * t : 128 * v + 64 * t + 64, :]))
            v2[at, :] = v1[at, :] - planes[256 * t : 256 * t + 256] - lines


def last_body(v2, *refs):
    zr, (ny, qzy, qy, out_far, fin, out, sem) = refs[:8], refs[8:]
    stats = merged_stats([r[80:88, :] for r in zr])
    lane = iota((8, 128), 1)
    step = COURANT / jnp.max(jnp.where(lane == VARS, stats, 0.0))
    norm = jnp.sqrt(stats * (1.0 / 16777216.0))
    for v in range(VARS):
        fin[v] = jnp.max(jnp.where(lane == v, norm, 0.0))
    copies = []
    for v in range(VARS):
        table = ny[v, 0:16, :]
        crossed = jnp.concatenate(
            [small_solve(table, [x[16 * v + 4 * r : 16 * v + 4 * r + 4, :] for x in zr])[0:4] for r in range(4)], axis=0
        )
        lines = dot1(qzy[v], stacked(crossed))
        for t in range(2):
            at = pl.ds(512 * v + 256 * t, 256)
            out[at, :] = step * (v2[at, :] + dot1(qy[v], stacked(lines[64 * t : 64 * t + 64])))
        at = pl.ds(512 * v, 512)
        copies.append(pltpu.make_async_copy(out.at[at], out_far.at[at], sem.at[v]))
        copies[v].start()
    for c in copies:
        c.wait()


def handed(x, axis):
    return lax.all_to_all(x, axis, 0, 0, tiled=True)


def shifted(x, axis, by):
    size = lax.axis_size(axis)
    return lax.ppermute(x, axis, [(i, (i + by) % size) for i in range(size)])


def swapped(x, axis, k):
    return lax.ppermute(x, axis, [(i, i ^ k) for i in range(lax.axis_size(axis))])


def shards(flow_state, advection, inverse_x, inverse_y, inverse_z, reduced_x, reduced_y, reduced_z):
    u = flow_state.reshape(2560, 128)
    xlo, xhi, ylo, yhi, zlo, zhi, keptx, kepty, keptz = call(
        faces_body,
        [((16, 512), F32)] * 2
        + [((320, 128), F32)] * 2
        + [((160, 128), F32)] * 2
        + [((5, 128, 128), F32), ((5, 16, 16), F32), ((5, 32, 32), F32)],
        (u, inverse_x, inverse_y, inverse_z),
    )
    from_zlo, from_zhi = shifted(zhi, "gz", 1), shifted(zlo, "gz", -1)
    from_ylo, from_yhi = shifted(yhi, "gy", 1), shifted(ylo, "gy", -1)
    from_xlo, from_xhi = shifted(xhi, "gx", 1), shifted(xlo, "gx", -1)
    ax, ay, az, qx = call(
        solve_tables_body,
        [((5, 384, 128), BF16), ((5, 128, 384), BF16), ((5, 256, 768), BF16), ((32, 128), F32)],
        (keptx, kepty, keptz),
    )
    w, bx = call(
        residual_body,
        [((2560, 128), F32), ((24, 512), F32)],
        (u, from_xlo, from_xhi, from_ylo, from_yhi, from_zlo, from_zhi, xlo, xhi, ax, ay, az),
        scratch=[
            ((180, 32, 128), F32),
            ((160, 32, 128), F32),
            ((170, 16, 128), F32),
            ((160, 16, 128), F32),
            ((512, 128), F32),
            ((512, 128), F32),
            ((128, 512), F32),
        ],
    )
    pieces = [bx] + [shifted(bx, "gx", k) for k in (1, 2, 3)]
    nx, ny, tz, mz = call(
        system_tables_body,
        [((32, 384), BF16), ((5, 32, 96), BF16), ((5, 32, 96), BF16), ((5, 32, 432), BF16)],
        (advection, reduced_x, reduced_y, reduced_z),
        smem=(0,),
    )
    v1, zp, mine, *own, give = call(
        spread_body,
        [((2560, 128), F32), ((1344, 128), F32), ((160, 128), F32)] + [((80, 128), F32)] * 4 + [((320, 128), F32)],
        (w, *pieces, nx, qx, tz),
        scratch=[((2560, 128), F32), ((128, 512), F32), ((640, 128), F32)],
        far_out=(0,),
        sems=5,
    )
    zr = handed(zp, "gz")
    yr = exchanged(own, give)
    *own, give = call(owners_body, [((80, 128), F32)] * 4 + [((320, 128), F32)], (*yr, ny))
    yg = exchanged(own, give)
    zy, zc, data = call(
        cross_body, [((88, 128), F32), ((320, 128), F32), ((640, 128), F32)], (zr, mine, mz, *yg)
    )
    lines = [zy, swapped(zy, "gy", 1)]
    for k in (2, 4, 6):
        lines.append(swapped(zy, "gy", k))
        lines.append(swapped(lines[-1], "gy", 1))
    qy, qz, qzy = call(
        column_tables_body,
        [((5, 256, 192), BF16), ((5, 256, 96), BF16), ((5, 128, 48), BF16)],
        (inverse_y, inverse_z),
        scratch=[((5, 16, 16), F32), ((5, 32, 32), F32)],
        far=(0, 1),
        sems=2,
    )
    (v2,) = call(
        middle_body,
        [((2560, 128), F32)],
        (v1, zc, data, qy, qz),
        scratch=[((2560, 128), F32)],
        far=(0,),
        sems=5,
    )
    out, fin = call(
        last_body,
        [((2560, 128), F32), ((VARS,), F32)],
        (v2, *lines, ny, qzy, qy),
        scratch=[((2560, 128), F32)],
        far_out=(0,),
        smem_out=(1,),
        sems=5,
    )
    return out.reshape(5, 32, 16, 128), fin


def solution(mesh):
    spec = P(None, "gz", "gy", "gx")
    return jax.shard_map(
        shards,
        mesh=mesh,
        in_specs=(spec, P(), P(), P(), P(), P(), P(), P()),
        out_specs=(spec, P()),
        check_vma=False,
    )
```

```python
import jax
import jax.numpy as jnp
from jax import lax
from jax.experimental import pallas as pl
from jax.experimental.pallas import tpu as pltpu
from jax.sharding import PartitionSpec as P


VARS = 5
F32 = jnp.float32
BF16 = jnp.bfloat16
DAMP = 0.0625
COURANT = 8000.0
VMEM = pltpu.VMEM
NN = (((1,), (0,)), ((), ()))


def iota(shape, dim):
    return lax.broadcasted_iota(jnp.int32, shape, dim)


def picks(shape, cond):
    return jnp.where(cond(iota(shape, 0), iota(shape, 1)), 1.0, 0.0).astype(BF16)


def split(x):
    hi = x.astype(BF16)
    return hi, (x - hi.astype(F32)).astype(BF16)


def dot1(a, b, dims=NN):
    return lax.dot_general(a, b, dims, preferred_element_type=F32)


def stacked(x):
    hi, lo = split(x)
    return jnp.concatenate([hi, hi, lo], axis=0)


def small_solve(table, pieces):
    return dot1(table, stacked(jnp.concatenate(pieces, axis=0)))


def call(body, out, args, scratch=(), far=(), smem=(), far_out=(), smem_out=(), sems=0, limit=24, flops=1_000_000):
    def spec(k, places):
        if k in smem and places is far:
            return pl.BlockSpec(memory_space=pltpu.SMEM)
        return pl.BlockSpec(memory_space=pltpu.HBM if k in places else VMEM)

    size = sum(a.size * a.dtype.itemsize for a in args)
    shapes = [VMEM(*t) for t in scratch]
    if sems:
        shapes.append(pltpu.SemaphoreType.DMA((sems,)))
    return pl.pallas_call(
        body,
        out_shape=[jax.ShapeDtypeStruct(*o) for o in out],
        in_specs=[spec(k, far) for k in range(len(args))],
        out_specs=[
            pl.BlockSpec(memory_space=pltpu.SMEM if k in smem_out else pltpu.HBM if k in far_out else VMEM)
            for k in range(len(out))
        ],
        scratch_shapes=shapes,
        compiler_params=pltpu.CompilerParams(vmem_limit_bytes=limit * 1024 * 1024),
        cost_estimate=pl.CostEstimate(flops=flops, bytes_accessed=size, transcendentals=0),
    )(*args)


def spread(left, parts, right, keep=None):
    wide = [dot1(dot1(left, part).astype(BF16), right) for part in parts]
    if keep is not None:
        wide = [jnp.where(keep, x, 0.0) for x in wide]
    return [x.astype(BF16) for x in wide]


def masked(shape, cond):
    return cond(iota(shape, 0), iota(shape, 1))


def put(ref, v, halves):
    hi, lo = halves
    k = hi.shape[1]
    ref[v, :, 0:k] = hi
    ref[v, :, k : 2 * k] = lo
    ref[v, :, 2 * k : 3 * k] = hi


def solve_tables_body(invy, invz, ay, az):
    y_left = picks((128, 16), lambda a, k: (a & 15) == k)
    y_right = picks((16, 128), lambda k, c: k == (c & 15))
    y_same = masked((128, 128), lambda a, c: (a >> 4) == (c >> 4))
    z_left = picks((256, 32), lambda a, k: (a >> 3) == k)
    z_right = picks((32, 256), lambda k, c: k == (c >> 3))
    z_same = masked((256, 256), lambda a, c: (a & 7) == (c & 7))
    for v in range(VARS):
        put(ay, v, spread(y_left, split(invy[v]), y_right, y_same))
        put(az, v, spread(z_left, split(invz[v]), z_right, z_same))


def first_off(r):
    return r - 2 + 4 * (r >> 1)


def second_off(r):
    return jnp.where(r == 0, -1, jnp.where(r == 3, 4, -4096))


def near(chosen, red, row, speed):
    hi, lo = split(red)
    both = dot1(chosen, hi) + dot1(chosen, lo)
    rows = both.shape[0] // 2
    other = jnp.where(row == 0, -0.5 * speed - 2.0, jnp.where(row == 3, 0.5 * speed - 2.0, 0.0))
    return 0.5 * both[0:rows] + other * both[rows:]


def exact(a, b):
    return lax.dot_general(a, b, NN, precision=lax.Precision.HIGHEST, preferred_element_type=F32)


def send_tables(adv, redx, redy, redz, nx, ty, tz):
    ix, iy, iz = lax.axis_index("gx"), lax.axis_index("gy"), lax.axis_index("gz")
    same = masked((32, 32), lambda a, c: (a & 7) == (c & 7))
    for out, red, at in ((ty, redy, iy), (tz, redz, iz)):
        left = picks((32, 32), lambda a, k: k == 4 * at + (a >> 3))
        right = picks((32, 32), lambda k, c: k == 4 * at + (c >> 3))
        for v in range(VARS):
            put(out, v, spread(left, split(red[v]), right, same))
    total = None
    row = (iota((32, 16), 0) & 3) ^ 2
    for v in range(VARS):
        chosen = jnp.concatenate(
            [
                picks((32, 16), lambda a, k, f=f: ((a >> 2) == v) & (k == 4 * ix + f((a & 3) ^ 2)))
                for f in (first_off, second_off)
            ],
            axis=0,
        )
        term = near(chosen, redx[v], row, adv[0, v])
        total = term if total is None else total + term
    right = picks((16, 128), lambda k, c: k == 4 * ((ix + 4 - (c >> 5)) & 3) + ((c & 3) ^ 2))
    same = masked((32, 128), lambda a, c: (a >> 2) == ((c >> 2) & 7))
    hi, lo = [jnp.where(same, dot1(part, right), 0.0).astype(BF16) for part in split(total)]
    nx[:, 0:128] = hi
    nx[:, 128:256] = lo
    nx[:, 256:384] = hi


def take_tables(adv, redy, redz, my, mz, ny, wide):
    row, lane = iota((32, 160), 0), iota((32, 160), 1)
    block, first = (lane >> 2) & 7, row - (lane & 28)
    low = (iota((8, 160), 0) & 3) < 2
    same = jnp.where((iota((160, 160), 0) >> 2) == (iota((160, 160), 1) >> 2), 1.0, 0.0)
    keep = masked((32, 432), lambda a, c: (a & 7) == (c & 7))
    left = picks((32, 8), lambda a, k: k == (a >> 3))
    third = iota((32, 432), 1)
    third, spot = jnp.where(third < 144, 0, jnp.where(third < 288, 1, 2)), third
    spot = (spot - 144 * third) >> 3
    spot = jnp.where(iota((32, 432), 0) == spot, 1.0, 0.0)
    ends, inner = jnp.where(third == 1, 0.0, spot).astype(BF16), jnp.where(third == 1, spot, 0.0).astype(BF16)
    source, column = iota((640, 160), 0), iota((640, 160), 1)
    part = jnp.where(source < 160, 0, jnp.where(source < 320, 1, jnp.where(source < 480, 2, 3)))
    inside = source - 160 * part
    for out, red, d, axis in ((my, redy, 1, "gy"), (mz, redz, 2, "gz")):
        at = lax.axis_index(axis)
        flip = at if axis == "gy" else 0
        for v in range(VARS):
            wide[:, 32 * v : 32 * v + 32] = red[v]
        table = wide[:, 0:160]
        start = jnp.where(block < at, 2, 0)
        here = block[0:8] == at

        def line(which):
            return jnp.sum(jnp.where(which, table, 0.0), axis=0, keepdims=True)

        a0, a1 = line(first == start), line(first == start + 1)
        e0, e1 = line(first == 2), line(first == 3)
        blank = jnp.zeros((2, 160), F32)
        sums = exact(jnp.concatenate([a0 * a0, a0 * a1, a1 * a1, e0 * e0, e0 * e1, e1 * e1, blank], axis=0), same)

        def dual(u0, u1, g):
            scale = 1.0 / (g[0:1] * g[2:3] - g[1:2] * g[1:2])
            return (g[2:3] * u0 - g[1:2] * u1) * scale, (g[0:1] * u1 - g[1:2] * u0) * scale

        p0, p1 = dual(a0, a1, sums[0:3])
        f0, f1 = dual(e0, e1, sums[3:6])
        chosen = jnp.concatenate(
            [picks((8, 32), lambda a, k, f=f: k == 4 * at + f(a & 3)) for f in (first_off, second_off)], axis=0
        )
        speed = jnp.zeros((8, 160), F32)
        for v in range(VARS):
            speed = jnp.where((iota((8, 160), 1) >> 5) == v, adv[d, v], speed)
        needed = near(chosen, table, iota((8, 160), 0) & 3, speed)
        sent = jnp.where(here & ~low, 0.0, needed)
        own = jnp.where(here & ~low, needed, 0.0)
        place = jnp.where(part < 2, 2 * (((inside >> 2) & 7) ^ flip), 14) + part
        gather = jnp.where(column == (inside & 224) + place, 1.0, 0.0)
        found = exact(jnp.concatenate([sent * p0, sent * p1, own * f0, own * f1], axis=1), gather)
        hi, lo = [dot1(left, x).astype(BF16) for x in split(found)]
        for v in range(VARS):
            at_v = slice(32 * v, 32 * v + 32)
            out[v] = jnp.where(keep, dot1(hi[:, at_v], ends) + dot1(lo[:, at_v], inner), 0.0).astype(BF16)
        if axis == "gy":
            wanted = iota((32, 96), 0) == 4 * (at ^ ((iota((32, 96), 1) >> 2) & 7)) + (iota((32, 96), 1) & 3)
            second = (iota((32, 96), 1) >> 5) == 1
            y_ends = jnp.where(wanted & ~second, 1.0, 0.0).astype(BF16)
            y_inner = jnp.where(wanted & second, 1.0, 0.0).astype(BF16)
            hi, lo = [jnp.concatenate([x, x], axis=0) for x in split(needed)]
            for v in range(VARS):
                at_v = slice(32 * v, 32 * v + 32)
                ny[v] = (dot1(hi[:, at_v], y_ends) + dot1(lo[:, at_v], y_inner)).astype(BF16)


def window_tables_body(adv, redx, redy, redz, invy, invz, nx, ty, tz, my, mz, ny, qy, qz, qzy, wide):
    send_tables(adv, redx, redy, redz, nx, ty, tz)
    take_tables(adv, redy, redz, my, mz, ny, wide)
    column_tables(invy, invz, qy, qz, qzy)


def column_tables(invy, invz, qy, qz, qzy):
    y_left = picks((128, 16), lambda a, k: (a & 15) == k)
    y_right = picks((16, 32), lambda k, c: k == (c >> 3) + 12 * (c >> 4))
    y_same = masked((128, 32), lambda a, c: (a >> 4) == (c & 7))
    z_left = picks((256, 32), lambda a, k: (a >> 3) == k)
    z_right = picks((32, 32), lambda k, c: k == (c >> 3) + 28 * (c >> 4))
    z_same = masked((256, 32), lambda a, c: (a & 7) == (c & 7))
    zy_left = picks((128, 32), lambda a, k: k == 8 * (a >> 5) + (a & 7))
    zy_right = picks((32, 16), lambda k, c: k == (c >> 2) + 28 * (c >> 3))
    zy_same = masked((128, 16), lambda a, c: ((a >> 3) & 3) == (c & 3))
    for v in range(VARS):
        put(qy, v, spread(y_left, split(invy[v]), y_right, y_same))
        parts = split(invz[v])
        put(qz, v, spread(z_left, parts, z_right, z_same))
        put(qzy, v, spread(zy_left, parts, zy_right, zy_same))


def faces_body(u, xlo, xhi, ylo, yhi, zlo, zhi):
    lane = iota((512, 128), 1)
    wide = jnp.zeros((512, 128), F32)
    for v in range(VARS):
        block = u[512 * v : 512 * v + 512, :]
        low = pltpu.roll(block, 2 * v, 1) if v else block
        wide = jnp.where((lane >> 1) == v, low, wide)
        wide = jnp.where((lane >> 1) == 8 + v, pltpu.roll(block, 18 + 2 * v, 1), wide)
        for j in range(2):
            at = 32 * (2 * v + j)
            ylo[at : at + 32, :] = u[pl.ds(512 * v + j, 32, stride=16), :]
            yhi[at : at + 32, :] = u[pl.ds(512 * v + 14 + j, 32, stride=16), :]
        zlo[32 * v : 32 * v + 32, :] = u[512 * v : 512 * v + 32, :]
        zhi[32 * v : 32 * v + 32, :] = u[512 * v + 480 : 512 * v + 512, :]
    turned = wide.T
    xlo[...] = turned[0:16]
    xhi[...] = turned[16:32]


def primitives(u):
    inverse = 1.0 / u[0]
    velocity = [u[1 + k] * inverse for k in range(3)]
    kinetic = 0.5 * (velocity[0] * velocity[0] + velocity[1] * velocity[1] + velocity[2] * velocity[2])
    internal = jnp.maximum(u[4] * inverse - kinetic, 0.25)
    return velocity, internal, 0.4 * u[0] * internal


def flux(u, velocity, pressure, d):
    w = velocity[d]
    out = [u[1 + d]]
    for k in range(3):
        moment = u[1 + k] * w
        out.append(moment + pressure if k == d else moment)
    out.append((u[4] + pressure) * w)
    return out


def stats_row(shape, sums, top):
    lane = iota(shape, len(shape) - 1)
    row = jnp.where(lane == VARS, top, 0.0)
    for v in range(VARS):
        row = jnp.where(lane == v, sums[v], row)
    return row


def merged_stats(rows):
    lane = iota(rows[0].shape, 1)
    total, top = rows[0], rows[0]
    for row in rows[1:]:
        total, top = total + row, jnp.maximum(top, row)
    return jnp.where(lane < VARS, total, top)


def residual_body(
    u, xlo, xhi, ylo, yhi, zlo, zhi, own_lo, own_hi, invx, ay, az, w, bx, qx, pad, fy, fz, res, fix, half, edge
):
    def fill(z, carry):
        for v in range(VARS):
            pad[36 * v + 2 + z, 8:24, :] = u[pl.ds(pl.multiple_of(512 * v + 16 * z, 16), 16), :]
        return carry

    lax.fori_loop(0, 32, fill, 0)
    rows = pad.reshape(180 * 32, 128)
    for v in range(VARS):
        for k in range(2):
            pad[36 * v + k, 8:24, :] = zlo[32 * v + 16 * k : 32 * v + 16 * k + 16, :]
            pad[36 * v + 34 + k, 8:24, :] = zhi[32 * v + 16 * k : 32 * v + 16 * k + 16, :]
            at = 32 * (2 * v + k)
            rows[pl.ds(32 * (36 * v + 2) + 6 + k, 32, stride=32), :] = ylo[at : at + 32, :]
            rows[pl.ds(32 * (36 * v + 2) + 24 + k, 32, stride=32), :] = yhi[at : at + 32, :]

    edge[...] = jnp.zeros_like(edge)

    def line(ref, j):
        return [ref[2 * v + j : 2 * v + j + 1, :] for v in range(VARS)]

    def fx(u):
        velocity, _, pressure = primitives(u)
        return flux(u, velocity, pressure, 0)

    l2, l1, h1, h2 = line(xlo, 0), line(xlo, 1), line(xhi, 0), line(xhi, 1)
    o0, o1, p1, p0 = line(own_lo, 0), line(own_lo, 1), line(own_hi, 0), line(own_hi, 1)
    fl, fp, fh, fo = fx(l1), fx(p0), fx(h1), fx(o0)
    for v in range(VARS):
        dl, dh = l1[v] - p0[v], h1[v] - o0[v]
        edge[4 * v : 4 * v + 1, :] = -DAMP * dh
        edge[4 * v + 1 : 4 * v + 2, :] = -0.5 * (fh[v] - fo[v]) + 4.0 * DAMP * dh - DAMP * (h2[v] - o1[v])
        edge[4 * v + 2 : 4 * v + 3, :] = 0.5 * (fl[v] - fp[v]) + 4.0 * DAMP * dl - DAMP * (l2[v] - p1[v])
        edge[4 * v + 3 : 4 * v + 4, :] = -DAMP * dl
    fix[...] = edge[...].T

    for z in (-1, 32):
        c = [pad[36 * v + 2 + z, 8:24, :] for v in range(VARS)]
        velocity, _, pressure = primitives(c)
        for v, f in enumerate(flux(c, velocity, pressure, 2)):
            fz[34 * v + 1 + z] = f

    def plane(z, top):
        full = [pad[36 * v + 2 + z] for v in range(VARS)]
        velocity, internal, pressure = primitives(full)
        for v, f in enumerate(flux(full, velocity, pressure, 1)):
            fy[32 * v + z] = f
        c = [f[8:24] for f in full]
        velocity, internal, pressure = [f[8:24] for f in velocity], internal[8:24], pressure[8:24]
        for v, f in enumerate(flux(c, velocity, pressure, 2)):
            fz[34 * v + 1 + z] = f
        for v, f in enumerate(flux(c, velocity, pressure, 0)):
            damped = (4.0 * DAMP) * c[v]
            res[32 * v + z] = (
                pltpu.roll(damped - 0.5 * f, 127, 1)
                + pltpu.roll(damped + 0.5 * f, 1, 1)
                - DAMP * (pltpu.roll(c[v], 126, 1) + pltpu.roll(c[v], 2, 1))
                - (18.0 * DAMP) * c[v]
            )
        speed = jnp.abs(velocity[0]) + jnp.abs(velocity[1]) + jnp.abs(velocity[2])
        return jnp.maximum(top, speed + jnp.sqrt((3.0 * 1.4 * 0.4) * internal))

    top = lax.fori_loop(0, 32, plane, jnp.zeros((16, 128), F32), unroll=2)

    lane = iota((16, 128), 1)
    edges = (lane < 2) | (lane >= 126)

    def finish(z, sums):
        out = []
        fixes = fix[pl.ds(pl.multiple_of(16 * z, 16), 16), :]
        for v in range(VARS):
            at = 36 * v + 2 + z
            ones = (pad[at, 7:23, :] + pad[at, 9:25, :]) + (pad[at - 1, 8:24, :] + pad[at + 1, 8:24, :])
            twos = (pad[at, 6:22, :] + pad[at, 10:26, :]) + (pad[at - 2, 8:24, :] + pad[at + 2, 8:24, :])
            steep = (fy[32 * v + z, 7:23, :] - fy[32 * v + z, 9:25, :]) + (fz[34 * v + z] - fz[34 * v + 2 + z])
            value = res[32 * v + z] + 0.5 * steep + (4.0 * DAMP) * ones - DAMP * twos
            value = value + jnp.where(edges, pltpu.roll(fixes, (126 - 4 * v) & 127, 1), 0.0)
            res[32 * v + z] = value
            out.append(sums[v] + value * value)
        return tuple(out)

    sums = lax.fori_loop(0, 32, finish, tuple(jnp.zeros((16, 128), F32) for _ in range(VARS)), unroll=2)

    qx[...] = jnp.zeros_like(qx)
    for v in range(VARS):
        turned = invx[v].T
        qx[4 * v : 4 * v + 2, :] = turned[126:128]
        qx[4 * v + 2 : 4 * v + 4, :] = turned[0:2]
        hi, lo = split(res[pl.ds(32 * v, 32)].reshape(512, 128))
        half[...] = dot1(jnp.concatenate([hi, lo, hi], axis=1), stacked(turned))
        for g in range(4):
            half[128 * g : 128 * g + 128, :] = dot1(ay[v], stacked(half[128 * g : 128 * g + 128, :]))
        field = half[...].reshape(32, 2, 8, 128)
        parts = [dot1(az[v], stacked(field[:, h].reshape(256, 128))).reshape(32, 1, 8, 128) for h in range(2)]
        w[pl.ds(pl.multiple_of(512 * v, 512), 512), :] = jnp.concatenate(parts, axis=1).reshape(512, 128)
    lane = iota((512, 128), 1)
    wide = jnp.zeros((512, 128), F32)
    for v in range(VARS):
        wide = jnp.where((lane >> 2) == v, pltpu.roll(w[512 * v : 512 * v + 512, :], 2 + 4 * v, 1), wide)
    turned = wide.T
    bx[...] = turned[0:24]
    bx[20:21, :] = stats_row((1, 512), [jnp.sum(s) for s in sums], jnp.max(top))


def spread_body(w, b0, b1, b2, b3, nx, qx, ty, tz, *rest):
    far, (mine, ydown, yup), towards, (v1, zp, wide, sem) = rest[:2], rest[2:5], rest[5:9], rest[9:]
    me, iz = lax.axis_index("gy"), lax.axis_index("gz")
    ups = [(me & 1) == 0] + [((me >> 1) ^ j) > (me >> 1) for j in (1, 2, 3)]
    blank = jnp.zeros((8, 512), F32)
    pieces = [b0, b1, b2, b3]
    data = jnp.concatenate([t for p in pieces for t in (p[...], blank)], axis=0)
    wide[...] = jnp.zeros_like(wide)
    wide[0:32, :] = dot1(nx[...], stacked(data))
    hi, lo = split(wide[...].T[:, 0:32])
    turned = jnp.concatenate([hi, lo, hi], axis=1)
    copies = []
    for v in range(VARS):
        at = pl.ds(512 * v, 512)
        hi, lo = split(jnp.where((iota((32, 128), 0) >> 2) == v, qx[...], 0.0))
        v1[at, :] = w[at, :] - dot1(turned, jnp.concatenate([hi, hi, lo], axis=0))
        copies.append(pltpu.make_async_copy(v1.at[at], far[0].at[at], sem.at[v]))
        copies[-1].start()
        for h in range(2):
            ends = [v1[512 * v + 16 * z + 8 * h : 512 * v + 16 * z + 8 * h + 8, :] for z in (0, 1, 30, 31)]
            sent = small_solve(tz[v], ends)
            at = 16 * (2 * v + h)
            mine[at : at + 16, :] = sent[16:32]
            for p in range(8):
                zp[p, at : at + 16, :] = jnp.where(p <= iz, sent[0:16], sent[16:32])
        for t in range(4):
            sent = small_solve(ty[v], [v1[pl.ds(512 * v + 128 * t + y, 8, stride=16), :] for y in (0, 1, 14, 15)])
            at = 16 * (4 * v + t)
            ydown[at : at + 16, :] = sent[0:16]
            yup[at : at + 16, :] = sent[16:32]
            for up, out in zip(ups, towards):
                out[at : at + 16, :] = jnp.where(up, sent[16:32], sent[0:16])
        at = pl.ds(32 * v, 32)
        copies.append(pltpu.make_async_copy(zp.at[:, at], far[1].at[:, at], sem.at[5 + v]))
        copies[-1].start()
    stats = jnp.broadcast_to(merged_stats([p[20:21, 0:128] for p in pieces]), (8, 128))
    for p in range(8):
        zp[p, 160:168, :] = stats
    at = pl.ds(160, 8)
    copies.append(pltpu.make_async_copy(zp.at[:, at], far[1].at[:, at], sem.at[10]))
    copies[-1].start()
    for c in copies:
        c.wait()


def cross_body(zr, mine, mz, *refs):
    zy, zc = refs[-2:]
    for v in range(VARS):
        for h in range(2):
            at = 16 * (2 * v + h)
            got = [zr[168 * q + at : 168 * q + at + 16, :] for q in range(8)] + [mine[at : at + 16, :]]
            zc[2 * at : 2 * at + 32, :] = small_solve(mz[v], got)
        for j, (h, y) in enumerate(((0, 0), (0, 1), (1, 6), (1, 7))):
            zy[pl.ds(16 * v + j, 4, stride=4), :] = zc[pl.ds(32 * (2 * v + h) + y, 4, stride=8), :]
    zy[80:88, :] = merged_stats([zr[168 * q + 160 : 168 * q + 168, :] for q in range(8)])


def middle_y_body(v1_far, my, qy, *refs):
    lines, (vy_far, v1, vy, sem) = refs[:9], refs[9:]
    copies, puts = [], []
    for v in range(VARS):
        at = pl.ds(512 * v, 512)
        copies.append(pltpu.make_async_copy(v1_far.at[at], v1.at[at], sem.at[v]))
        puts.append(pltpu.make_async_copy(vy.at[at], vy_far.at[at], sem.at[5 + v]))
        copies[v].start()
    for v in range(VARS):
        copies[v].wait()
        for t in range(4):
            at = 16 * (4 * v + t)
            found = small_solve(my[v], [x[at : at + 16, :] for x in lines])
            at = pl.ds(512 * v + 128 * t, 128)
            vy[at, :] = v1[at, :] - dot1(qy[v], stacked(found))
        puts[v].start()
    for c in puts:
        c.wait()


def middle_z_body(vy_far, zc, qz, v2, vy, sem):
    copies = []
    for v in range(VARS):
        at = pl.ds(512 * v, 512)
        copies.append(pltpu.make_async_copy(vy_far.at[at], vy.at[at], sem.at[v]))
        copies[v].start()
    for v in range(VARS):
        parts = []
        for h in range(2):
            rows = zc[64 * v + 32 * h : 64 * v + 32 * h + 32, :]
            parts.append(dot1(qz[v], stacked(rows)).reshape(32, 1, 8, 128))
        planes = jnp.concatenate(parts, axis=1).reshape(512, 128)
        copies[v].wait()
        at = pl.ds(512 * v, 512)
        v2[at, :] = vy[at, :] - planes


def last_body(v2, *refs):
    zr, (ny, qzy, qy, out_far, fin, out, sem) = refs[:8], refs[8:]
    stats = merged_stats([r[80:88, :] for r in zr])
    lane = iota((8, 128), 1)
    step = COURANT / jnp.max(jnp.where(lane == VARS, stats, 0.0))
    norm = jnp.sqrt(stats * (1.0 / 16777216.0))
    for v in range(VARS):
        fin[v] = jnp.max(jnp.where(lane == v, norm, 0.0))
    copies = []
    for v in range(VARS):
        table = ny[v]
        crossed = jnp.concatenate(
            [small_solve(table, [x[16 * v + 4 * r : 16 * v + 4 * r + 4, :] for x in zr])[0:4] for r in range(4)], axis=0
        )
        lines = dot1(qzy[v], stacked(crossed))
        for t in range(4):
            at = pl.ds(512 * v + 128 * t, 128)
            out[at, :] = step * (v2[at, :] + dot1(qy[v], stacked(lines[32 * t : 32 * t + 32])))
        at = pl.ds(512 * v, 512)
        copies.append(pltpu.make_async_copy(out.at[at], out_far.at[at], sem.at[v]))
        copies[v].start()
    for c in copies:
        c.wait()


def handed(x, axis):
    return lax.all_to_all(x, axis, 0, 0, tiled=True)


def shifted(x, axis, by):
    size = lax.axis_size(axis)
    return lax.ppermute(x, axis, [(i, (i + by) % size) for i in range(size)])


def swapped(x, axis, k):
    return lax.ppermute(x, axis, [(i, i ^ k) for i in range(lax.axis_size(axis))])


def step(flow_state, advection, inverse_x, inverse_y, inverse_z, reduced_x, reduced_y, reduced_z):
    u = flow_state.reshape(2560, 128)
    xlo, xhi, ylo, yhi, zlo, zhi = call(
        faces_body, [((16, 512), F32)] * 2 + [((320, 128), F32)] * 2 + [((160, 128), F32)] * 2, (u,)
    )
    from_zlo, from_zhi = shifted(zhi, "gz", 1), shifted(zlo, "gz", -1)
    from_ylo, from_yhi = shifted(yhi, "gy", 1), shifted(ylo, "gy", -1)
    from_xlo, from_xhi = shifted(xhi, "gx", 1), shifted(xlo, "gx", -1)
    ay, az = call(solve_tables_body, [((5, 128, 384), BF16), ((5, 256, 768), BF16)], (inverse_y, inverse_z))
    w, bx, qx = call(
        residual_body,
        [((2560, 128), F32), ((24, 512), F32), ((32, 128), F32)],
        (u, from_xlo, from_xhi, from_ylo, from_yhi, from_zlo, from_zhi, xlo, xhi, inverse_x, ay, az),
        scratch=[
            ((180, 32, 128), F32),
            ((160, 32, 128), F32),
            ((170, 16, 128), F32),
            ((160, 16, 128), F32),
            ((512, 128), F32),
            ((512, 128), F32),
            ((128, 512), F32),
        ],
    )
    pieces = [bx] + [shifted(bx, "gx", k) for k in (1, 2, 3)]
    nx, ty, tz, my, mz, ny, qy, qz, qzy = call(
        window_tables_body,
        [
            ((32, 384), BF16),
            ((5, 32, 96), BF16),
            ((5, 32, 96), BF16),
            ((5, 32, 432), BF16),
            ((5, 32, 432), BF16),
            ((5, 16, 96), BF16),
            ((5, 128, 96), BF16),
            ((5, 256, 96), BF16),
            ((5, 128, 48), BF16),
        ],
        (advection, reduced_x, reduced_y, reduced_z, inverse_y, inverse_z),
        scratch=[((32, 256), F32)],
        smem=(0,),
    )
    big, tall, flat = ((2560, 128), F32), ((8, 168, 128), F32), ((320, 128), F32)
    v1, zp, mine, ydown, yup, pair, *chips = call(
        spread_body,
        [big, tall, ((160, 128), F32)] + [flat] * 6,
        (w, *pieces, nx, qx, ty, tz),
        scratch=[big, tall, ((128, 512), F32)],
        far_out=(0, 1),
        sems=11,
    )
    zr = handed(zp, "gz").reshape(1344, 128)
    lines = [ydown, swapped(pair, "gy", 1)]
    for j in (1, 2, 3):
        lines.append(swapped(chips[j - 1], "gy", 2 * j))
        lines.append(swapped(lines[-1], "gy", 1))
    lines.append(yup)
    (vy,) = call(
        middle_y_body,
        [big],
        (v1, my, qy, *lines),
        scratch=[big, big],
        far=(0,),
        far_out=(0,),
        sems=10,
    )
    zy, zc = call(
        cross_body, [((88, 128), F32), ((320, 128), F32)], (zr, mine, mz, vy), far=(3,)
    )
    crossed = [zy, swapped(zy, "gy", 1)]
    for k in (2, 4, 6):
        crossed.append(swapped(zy, "gy", k))
        crossed.append(swapped(crossed[-1], "gy", 1))
    (v2,) = call(middle_z_body, [big], (vy, zc, qz), scratch=[big], far=(0,), sems=5)
    out, fin = call(
        last_body,
        [((2560, 128), F32), ((VARS,), F32)],
        (v2, *crossed, ny, qzy, qy),
        scratch=[((2560, 128), F32)],
        far_out=(0,),
        smem_out=(1,),
        sems=5,
    )
    return out.reshape(5, 32, 16, 128), fin


def solution(mesh):
    spec = P(None, "gz", "gy", "gx")
    return jax.shard_map(
        step,
        mesh=mesh,
        in_specs=(spec, P(), P(), P(), P(), P(), P(), P()),
        out_specs=(spec, P()),
        check_vma=False,
    )
```

```python
import jax
import jax.numpy as jnp
from jax import lax
from jax.experimental import pallas as pl
from jax.experimental.pallas import tpu as pltpu
from jax.sharding import PartitionSpec as P


VARS = 5
F32 = jnp.float32
BF16 = jnp.bfloat16
DAMP = 0.0625
COURANT = 8000.0
VMEM = pltpu.VMEM
NN = (((1,), (0,)), ((), ()))


def iota(shape, dim):
    return lax.broadcasted_iota(jnp.int32, shape, dim)


def picks(shape, cond):
    return jnp.where(cond(iota(shape, 0), iota(shape, 1)), 1.0, 0.0).astype(BF16)


def split(x):
    hi = x.astype(BF16)
    return hi, (x - hi.astype(F32)).astype(BF16)


def dot1(a, b, dims=NN):
    return lax.dot_general(a, b, dims, preferred_element_type=F32)


def stacked(x):
    hi, lo = split(x)
    return jnp.concatenate([hi, hi, lo], axis=0)


def small_solve(table, pieces):
    return dot1(table, stacked(jnp.concatenate(pieces, axis=0)))


def call(body, out, args, scratch=(), far=(), smem=(), far_out=(), smem_out=(), sems=0, limit=24, flops=1_000_000):
    def spec(k, places):
        if k in smem and places is far:
            return pl.BlockSpec(memory_space=pltpu.SMEM)
        return pl.BlockSpec(memory_space=pltpu.HBM if k in places else VMEM)

    size = sum(a.size * a.dtype.itemsize for a in args)
    shapes = [VMEM(*t) for t in scratch]
    if sems:
        shapes.append(pltpu.SemaphoreType.DMA((sems,)))
    return pl.pallas_call(
        body,
        out_shape=[jax.ShapeDtypeStruct(*o) for o in out],
        in_specs=[spec(k, far) for k in range(len(args))],
        out_specs=[
            pl.BlockSpec(memory_space=pltpu.SMEM if k in smem_out else pltpu.HBM if k in far_out else VMEM)
            for k in range(len(out))
        ],
        scratch_shapes=shapes,
        compiler_params=pltpu.CompilerParams(vmem_limit_bytes=limit * 1024 * 1024),
        cost_estimate=pl.CostEstimate(flops=flops, bytes_accessed=size, transcendentals=0),
    )(*args)


def spread(left, parts, right, keep=None):
    wide = [dot1(dot1(left, part).astype(BF16), right) for part in parts]
    if keep is not None:
        wide = [jnp.where(keep, x, 0.0) for x in wide]
    return [x.astype(BF16) for x in wide]


def masked(shape, cond):
    return cond(iota(shape, 0), iota(shape, 1))


def put(ref, v, halves):
    hi, lo = halves
    k = hi.shape[1]
    ref[v, :, 0:k] = hi
    ref[v, :, k : 2 * k] = lo
    ref[v, :, 2 * k : 3 * k] = hi


def solve_tables_body(invy, invz, ay, az):
    y_left = picks((128, 16), lambda a, k: (a & 15) == k)
    y_right = picks((16, 128), lambda k, c: k == (c & 15))
    y_same = masked((128, 128), lambda a, c: (a >> 4) == (c >> 4))
    z_left = picks((256, 32), lambda a, k: (a >> 3) == k)
    z_right = picks((32, 256), lambda k, c: k == (c >> 3))
    z_same = masked((256, 256), lambda a, c: (a & 7) == (c & 7))
    for v in range(VARS):
        put(ay, v, spread(y_left, split(invy[v]), y_right, y_same))
        put(az, v, spread(z_left, split(invz[v]), z_right, z_same))


def first_off(r):
    return r - 2 + 4 * (r >> 1)


def second_off(r):
    return jnp.where(r == 0, -1, jnp.where(r == 3, 4, -4096))


def near(chosen, red, row, speed):
    hi, lo = split(red)
    both = dot1(chosen, hi) + dot1(chosen, lo)
    rows = both.shape[0] // 2
    other = jnp.where(row == 0, -0.5 * speed - 2.0, jnp.where(row == 3, 0.5 * speed - 2.0, 0.0))
    return 0.5 * both[0:rows] + other * both[rows:]


def exact(a, b):
    return lax.dot_general(a, b, NN, precision=lax.Precision.HIGHEST, preferred_element_type=F32)


def send_tables(adv, redx, redy, redz, nx, ty, tz):
    ix, iy, iz = lax.axis_index("gx"), lax.axis_index("gy"), lax.axis_index("gz")
    same = masked((32, 32), lambda a, c: (a & 7) == (c & 7))
    for out, red, at in ((ty, redy, iy), (tz, redz, iz)):
        left = picks((32, 32), lambda a, k: k == 4 * at + (a >> 3))
        right = picks((32, 32), lambda k, c: k == 4 * at + (c >> 3))
        for v in range(VARS):
            put(out, v, spread(left, split(red[v]), right, same))
    total = None
    row = (iota((32, 16), 0) & 3) ^ 2
    for v in range(VARS):
        chosen = jnp.concatenate(
            [
                picks((32, 16), lambda a, k, f=f: ((a >> 2) == v) & (k == 4 * ix + f((a & 3) ^ 2)))
                for f in (first_off, second_off)
            ],
            axis=0,
        )
        term = near(chosen, redx[v], row, adv[0, v])
        total = term if total is None else total + term
    right = picks((16, 128), lambda k, c: k == 4 * ((ix + 4 - (c >> 5)) & 3) + ((c & 3) ^ 2))
    same = masked((32, 128), lambda a, c: (a >> 2) == ((c >> 2) & 7))
    hi, lo = [jnp.where(same, dot1(part, right), 0.0).astype(BF16) for part in split(total)]
    nx[:, 0:128] = hi
    nx[:, 128:256] = lo
    nx[:, 256:384] = hi


def take_tables(adv, redy, redz, my, mz, ny, wide):
    row, lane = iota((32, 160), 0), iota((32, 160), 1)
    block, first = (lane >> 2) & 7, row - (lane & 28)
    low = (iota((8, 160), 0) & 3) < 2
    same = jnp.where((iota((160, 160), 0) >> 2) == (iota((160, 160), 1) >> 2), 1.0, 0.0)
    keep = masked((32, 432), lambda a, c: (a & 7) == (c & 7))
    left = picks((32, 8), lambda a, k: k == (a >> 3))
    third = iota((32, 432), 1)
    third, spot = jnp.where(third < 144, 0, jnp.where(third < 288, 1, 2)), third
    spot = (spot - 144 * third) >> 3
    spot = jnp.where(iota((32, 432), 0) == spot, 1.0, 0.0)
    ends, inner = jnp.where(third == 1, 0.0, spot).astype(BF16), jnp.where(third == 1, spot, 0.0).astype(BF16)
    source, column = iota((640, 160), 0), iota((640, 160), 1)
    part = jnp.where(source < 160, 0, jnp.where(source < 320, 1, jnp.where(source < 480, 2, 3)))
    inside = source - 160 * part
    for out, red, d, axis in ((my, redy, 1, "gy"), (mz, redz, 2, "gz")):
        at = lax.axis_index(axis)
        flip = at if axis == "gy" else 0
        for v in range(VARS):
            wide[:, 32 * v : 32 * v + 32] = red[v]
        table = wide[:, 0:160]
        start = jnp.where(block < at, 2, 0)
        here = block[0:8] == at

        def line(which):
            return jnp.sum(jnp.where(which, table, 0.0), axis=0, keepdims=True)

        a0, a1 = line(first == start), line(first == start + 1)
        e0, e1 = line(first == 2), line(first == 3)
        blank = jnp.zeros((2, 160), F32)
        sums = exact(jnp.concatenate([a0 * a0, a0 * a1, a1 * a1, e0 * e0, e0 * e1, e1 * e1, blank], axis=0), same)

        def dual(u0, u1, g):
            scale = 1.0 / (g[0:1] * g[2:3] - g[1:2] * g[1:2])
            return (g[2:3] * u0 - g[1:2] * u1) * scale, (g[0:1] * u1 - g[1:2] * u0) * scale

        p0, p1 = dual(a0, a1, sums[0:3])
        f0, f1 = dual(e0, e1, sums[3:6])
        chosen = jnp.concatenate(
            [picks((8, 32), lambda a, k, f=f: k == 4 * at + f(a & 3)) for f in (first_off, second_off)], axis=0
        )
        speed = jnp.zeros((8, 160), F32)
        for v in range(VARS):
            speed = jnp.where((iota((8, 160), 1) >> 5) == v, adv[d, v], speed)
        needed = near(chosen, table, iota((8, 160), 0) & 3, speed)
        sent = jnp.where(here & ~low, 0.0, needed)
        own = jnp.where(here & ~low, needed, 0.0)
        place = jnp.where(part < 2, 2 * (((inside >> 2) & 7) ^ flip), 14) + part
        gather = jnp.where(column == (inside & 224) + place, 1.0, 0.0)
        found = exact(jnp.concatenate([sent * p0, sent * p1, own * f0, own * f1], axis=1), gather)
        hi, lo = [dot1(left, x).astype(BF16) for x in split(found)]
        for v in range(VARS):
            at_v = slice(32 * v, 32 * v + 32)
            out[v] = jnp.where(keep, dot1(hi[:, at_v], ends) + dot1(lo[:, at_v], inner), 0.0).astype(BF16)
        if axis == "gy":
            wanted = iota((32, 96), 0) == 4 * (at ^ ((iota((32, 96), 1) >> 2) & 7)) + (iota((32, 96), 1) & 3)
            second = (iota((32, 96), 1) >> 5) == 1
            y_ends = jnp.where(wanted & ~second, 1.0, 0.0).astype(BF16)
            y_inner = jnp.where(wanted & second, 1.0, 0.0).astype(BF16)
            hi, lo = [jnp.concatenate([x, x], axis=0) for x in split(needed)]
            for v in range(VARS):
                at_v = slice(32 * v, 32 * v + 32)
                ny[v] = (dot1(hi[:, at_v], y_ends) + dot1(lo[:, at_v], y_inner)).astype(BF16)


def window_tables_body(adv, redx, redy, redz, invy, invz, nx, ty, tz, my, mz, ny, qy, qz, qzy, wide):
    send_tables(adv, redx, redy, redz, nx, ty, tz)
    take_tables(adv, redy, redz, my, mz, ny, wide)
    column_tables(invy, invz, qy, qz, qzy)


def column_tables(invy, invz, qy, qz, qzy):
    y_left = picks((128, 16), lambda a, k: (a & 15) == k)
    y_right = picks((16, 32), lambda k, c: k == (c >> 3) + 12 * (c >> 4))
    y_same = masked((128, 32), lambda a, c: (a >> 4) == (c & 7))
    z_left = picks((256, 32), lambda a, k: (a >> 3) == k)
    z_right = picks((32, 32), lambda k, c: k == (c >> 3) + 28 * (c >> 4))
    z_same = masked((256, 32), lambda a, c: (a & 7) == (c & 7))
    zy_left = picks((128, 32), lambda a, k: k == 8 * (a >> 5) + (a & 7))
    zy_right = picks((32, 16), lambda k, c: k == (c >> 2) + 28 * (c >> 3))
    zy_same = masked((128, 16), lambda a, c: ((a >> 3) & 3) == (c & 3))
    for v in range(VARS):
        put(qy, v, spread(y_left, split(invy[v]), y_right, y_same))
        parts = split(invz[v])
        put(qz, v, spread(z_left, parts, z_right, z_same))
        put(qzy, v, spread(zy_left, parts, zy_right, zy_same))


def faces_body(u, xlo, xhi, ylo, yhi, zlo, zhi):
    lane = iota((512, 128), 1)
    wide = jnp.zeros((512, 128), F32)
    for v in range(VARS):
        block = u[512 * v : 512 * v + 512, :]
        low = pltpu.roll(block, 2 * v, 1) if v else block
        wide = jnp.where((lane >> 1) == v, low, wide)
        wide = jnp.where((lane >> 1) == 8 + v, pltpu.roll(block, 18 + 2 * v, 1), wide)
        for j in range(2):
            at = 32 * (2 * v + j)
            ylo[at : at + 32, :] = u[pl.ds(512 * v + j, 32, stride=16), :]
            yhi[at : at + 32, :] = u[pl.ds(512 * v + 14 + j, 32, stride=16), :]
        zlo[32 * v : 32 * v + 32, :] = u[512 * v : 512 * v + 32, :]
        zhi[32 * v : 32 * v + 32, :] = u[512 * v + 480 : 512 * v + 512, :]
    turned = wide.T
    xlo[...] = turned[0:16]
    xhi[...] = turned[16:32]


def primitives(u):
    inverse = 1.0 / u[0]
    velocity = [u[1 + k] * inverse for k in range(3)]
    kinetic = 0.5 * (velocity[0] * velocity[0] + velocity[1] * velocity[1] + velocity[2] * velocity[2])
    internal = jnp.maximum(u[4] * inverse - kinetic, 0.25)
    return velocity, internal, 0.4 * u[0] * internal


def flux(u, velocity, pressure, d):
    w = velocity[d]
    out = [u[1 + d]]
    for k in range(3):
        moment = u[1 + k] * w
        out.append(moment + pressure if k == d else moment)
    out.append((u[4] + pressure) * w)
    return out


def stats_row(shape, sums, top):
    lane = iota(shape, len(shape) - 1)
    row = jnp.where(lane == VARS, top, 0.0)
    for v in range(VARS):
        row = jnp.where(lane == v, sums[v], row)
    return row


def merged_stats(rows):
    lane = iota(rows[0].shape, 1)
    total, top = rows[0], rows[0]
    for row in rows[1:]:
        total, top = total + row, jnp.maximum(top, row)
    return jnp.where(lane < VARS, total, top)


def residual_body(
    u, xlo, xhi, ylo, yhi, zlo, zhi, own_lo, own_hi, invx, ay, az, w, bx, qx, pad, fy, fz, res, fix, half, edge
):
    def fill(z, carry):
        for v in range(VARS):
            pad[36 * v + 2 + z, 8:24, :] = u[pl.ds(pl.multiple_of(512 * v + 16 * z, 16), 16), :]
        return carry

    lax.fori_loop(0, 32, fill, 0)
    rows = pad.reshape(180 * 32, 128)
    for v in range(VARS):
        for k in range(2):
            pad[36 * v + k, 8:24, :] = zlo[32 * v + 16 * k : 32 * v + 16 * k + 16, :]
            pad[36 * v + 34 + k, 8:24, :] = zhi[32 * v + 16 * k : 32 * v + 16 * k + 16, :]
            at = 32 * (2 * v + k)
            rows[pl.ds(32 * (36 * v + 2) + 6 + k, 32, stride=32), :] = ylo[at : at + 32, :]
            rows[pl.ds(32 * (36 * v + 2) + 24 + k, 32, stride=32), :] = yhi[at : at + 32, :]

    edge[...] = jnp.zeros_like(edge)

    def line(ref, j):
        return [ref[2 * v + j : 2 * v + j + 1, :] for v in range(VARS)]

    def fx(u):
        velocity, _, pressure = primitives(u)
        return flux(u, velocity, pressure, 0)

    l2, l1, h1, h2 = line(xlo, 0), line(xlo, 1), line(xhi, 0), line(xhi, 1)
    o0, o1, p1, p0 = line(own_lo, 0), line(own_lo, 1), line(own_hi, 0), line(own_hi, 1)
    fl, fp, fh, fo = fx(l1), fx(p0), fx(h1), fx(o0)
    for v in range(VARS):
        dl, dh = l1[v] - p0[v], h1[v] - o0[v]
        edge[4 * v : 4 * v + 1, :] = -DAMP * dh
        edge[4 * v + 1 : 4 * v + 2, :] = -0.5 * (fh[v] - fo[v]) + 4.0 * DAMP * dh - DAMP * (h2[v] - o1[v])
        edge[4 * v + 2 : 4 * v + 3, :] = 0.5 * (fl[v] - fp[v]) + 4.0 * DAMP * dl - DAMP * (l2[v] - p1[v])
        edge[4 * v + 3 : 4 * v + 4, :] = -DAMP * dl
    fix[...] = edge[...].T

    for z in (-1, 32):
        c = [pad[36 * v + 2 + z, 8:24, :] for v in range(VARS)]
        velocity, _, pressure = primitives(c)
        for v, f in enumerate(flux(c, velocity, pressure, 2)):
            fz[34 * v + 1 + z] = f

    def plane(z, top):
        full = [pad[36 * v + 2 + z] for v in range(VARS)]
        velocity, internal, pressure = primitives(full)
        for v, f in enumerate(flux(full, velocity, pressure, 1)):
            fy[32 * v + z] = f
        c = [f[8:24] for f in full]
        velocity, internal, pressure = [f[8:24] for f in velocity], internal[8:24], pressure[8:24]
        for v, f in enumerate(flux(c, velocity, pressure, 2)):
            fz[34 * v + 1 + z] = f
        for v, f in enumerate(flux(c, velocity, pressure, 0)):
            damped = (4.0 * DAMP) * c[v]
            res[32 * v + z] = (
                pltpu.roll(damped - 0.5 * f, 127, 1)
                + pltpu.roll(damped + 0.5 * f, 1, 1)
                - DAMP * (pltpu.roll(c[v], 126, 1) + pltpu.roll(c[v], 2, 1))
                - (18.0 * DAMP) * c[v]
            )
        speed = jnp.abs(velocity[0]) + jnp.abs(velocity[1]) + jnp.abs(velocity[2])
        return jnp.maximum(top, speed + jnp.sqrt((3.0 * 1.4 * 0.4) * internal))

    top = lax.fori_loop(0, 32, plane, jnp.zeros((16, 128), F32), unroll=4)

    lane = iota((16, 128), 1)
    edges = (lane < 2) | (lane >= 126)

    def finish(z, sums):
        out = []
        fixes = fix[pl.ds(pl.multiple_of(16 * z, 16), 16), :]
        for v in range(VARS):
            at = 36 * v + 2 + z
            ones = (pad[at, 7:23, :] + pad[at, 9:25, :]) + (pad[at - 1, 8:24, :] + pad[at + 1, 8:24, :])
            twos = (pad[at, 6:22, :] + pad[at, 10:26, :]) + (pad[at - 2, 8:24, :] + pad[at + 2, 8:24, :])
            steep = (fy[32 * v + z, 7:23, :] - fy[32 * v + z, 9:25, :]) + (fz[34 * v + z] - fz[34 * v + 2 + z])
            value = res[32 * v + z] + 0.5 * steep + (4.0 * DAMP) * ones - DAMP * twos
            value = value + jnp.where(edges, pltpu.roll(fixes, (126 - 4 * v) & 127, 1), 0.0)
            res[32 * v + z] = value
            out.append(sums[v] + value * value)
        return tuple(out)

    sums = lax.fori_loop(0, 32, finish, tuple(jnp.zeros((16, 128), F32) for _ in range(VARS)), unroll=2)

    qx[...] = jnp.zeros_like(qx)
    for v in range(VARS):
        turned = invx[v].T
        qx[4 * v : 4 * v + 2, :] = turned[126:128]
        qx[4 * v + 2 : 4 * v + 4, :] = turned[0:2]
        hi, lo = split(res[pl.ds(32 * v, 32)].reshape(512, 128))
        half[...] = dot1(jnp.concatenate([hi, lo, hi], axis=1), stacked(turned))
        for g in range(4):
            half[128 * g : 128 * g + 128, :] = dot1(ay[v], stacked(half[128 * g : 128 * g + 128, :]))
        field = half[...].reshape(32, 2, 8, 128)
        parts = [dot1(az[v], stacked(field[:, h].reshape(256, 128))).reshape(32, 1, 8, 128) for h in range(2)]
        w[pl.ds(pl.multiple_of(512 * v, 512), 512), :] = jnp.concatenate(parts, axis=1).reshape(512, 128)
    lane = iota((512, 128), 1)
    wide = jnp.zeros((512, 128), F32)
    for v in range(VARS):
        wide = jnp.where((lane >> 2) == v, pltpu.roll(w[512 * v : 512 * v + 512, :], 2 + 4 * v, 1), wide)
    turned = wide.T
    bx[...] = turned[0:24]
    bx[20:21, :] = stats_row((1, 512), [jnp.sum(s) for s in sums], jnp.max(top))


def spread_body(w, b0, b1, b2, b3, nx, qx, ty, tz, *rest):
    far, mine, towards, (v1, zp, wide, sem) = rest[:2], rest[2], rest[3:7], rest[7:]
    me, iz = lax.axis_index("gy"), lax.axis_index("gz")
    ups = [(me & 1) == 0] + [((me >> 1) ^ j) > (me >> 1) for j in (1, 2, 3)]
    blank = jnp.zeros((8, 512), F32)
    pieces = [b0, b1, b2, b3]
    data = jnp.concatenate([t for p in pieces for t in (p[...], blank)], axis=0)
    wide[...] = jnp.zeros_like(wide)
    wide[0:32, :] = dot1(nx[...], stacked(data))
    hi, lo = split(wide[...].T[:, 0:32])
    turned = jnp.concatenate([hi, lo, hi], axis=1)
    copies = []
    for v in range(VARS):
        at = pl.ds(512 * v, 512)
        hi, lo = split(jnp.where((iota((32, 128), 0) >> 2) == v, qx[...], 0.0))
        v1[at, :] = w[at, :] - dot1(turned, jnp.concatenate([hi, hi, lo], axis=0))
        copies.append(pltpu.make_async_copy(v1.at[at], far[0].at[at], sem.at[v]))
        copies[-1].start()
        for h in range(2):
            ends = [v1[512 * v + 16 * z + 8 * h : 512 * v + 16 * z + 8 * h + 8, :] for z in (0, 1, 30, 31)]
            sent = small_solve(tz[v], ends)
            at = 16 * (2 * v + h)
            mine[at : at + 16, :] = sent[16:32]
            for p in range(8):
                zp[p, at : at + 16, :] = jnp.where(p <= iz, sent[0:16], sent[16:32])
        for t in range(4):
            sent = small_solve(ty[v], [v1[pl.ds(512 * v + 128 * t + y, 8, stride=16), :] for y in (0, 1, 14, 15)])
            at = 16 * (4 * v + t)
            for up, out in zip(ups, towards):
                out[at : at + 16, :] = jnp.where(up, sent[16:32], sent[0:16])
        at = pl.ds(32 * v, 32)
        copies.append(pltpu.make_async_copy(zp.at[:, at], far[1].at[:, at], sem.at[5 + v]))
        copies[-1].start()
    stats = jnp.broadcast_to(merged_stats([p[20:21, 0:128] for p in pieces]), (8, 128))
    for p in range(8):
        zp[p, 160:168, :] = stats
    at = pl.ds(160, 8)
    copies.append(pltpu.make_async_copy(zp.at[:, at], far[1].at[:, at], sem.at[10]))
    copies[-1].start()
    for c in copies:
        c.wait()


def cross_body(zr, mine, mz, *refs):
    zy, zc = refs[-2:]
    for v in range(VARS):
        for h in range(2):
            at = 16 * (2 * v + h)
            got = [zr[168 * q + at : 168 * q + at + 16, :] for q in range(8)] + [mine[at : at + 16, :]]
            zc[2 * at : 2 * at + 32, :] = small_solve(mz[v], got)
        for j, (h, y) in enumerate(((0, 0), (0, 1), (1, 6), (1, 7))):
            zy[pl.ds(16 * v + j, 4, stride=4), :] = zc[pl.ds(32 * (2 * v + h) + y, 4, stride=8), :]
    zy[80:88, :] = merged_stats([zr[168 * q + 160 : 168 * q + 168, :] for q in range(8)])


def own_body(v1_far, ty, down, up, v1, sem):
    copies = []
    for v in range(VARS):
        at = pl.ds(512 * v, 512)
        copies.append(pltpu.make_async_copy(v1_far.at[at], v1.at[at], sem.at[v]))
        copies[v].start()
    for v in range(VARS):
        copies[v].wait()
        for t in range(4):
            own = small_solve(ty[v], [v1[pl.ds(512 * v + 128 * t + y, 8, stride=16), :] for y in (0, 1, 14, 15)])
            at = 16 * (4 * v + t)
            down[at : at + 16, :] = own[0:16]
            up[at : at + 16, :] = own[16:32]


def middle_y_body(v1_far, my, qy, *refs):
    lines, (vy_far, v1, vy, sem) = refs[:9], refs[9:]
    copies, puts = [], []
    for v in range(VARS):
        at = pl.ds(512 * v, 512)
        copies.append(pltpu.make_async_copy(v1_far.at[at], v1.at[at], sem.at[v]))
        puts.append(pltpu.make_async_copy(vy.at[at], vy_far.at[at], sem.at[5 + v]))
        copies[v].start()
    for v in range(VARS):
        copies[v].wait()
        for t in range(4):
            at = 16 * (4 * v + t)
            found = small_solve(my[v], [x[at : at + 16, :] for x in lines])
            at = pl.ds(512 * v + 128 * t, 128)
            vy[at, :] = v1[at, :] - dot1(qy[v], stacked(found))
        puts[v].start()
    for c in puts:
        c.wait()


def middle_z_body(vy_far, zc, qz, v2, vy, sem):
    copies = []
    for v in range(VARS):
        at = pl.ds(512 * v, 512)
        copies.append(pltpu.make_async_copy(vy_far.at[at], vy.at[at], sem.at[v]))
        copies[v].start()
    for v in range(VARS):
        parts = []
        for h in range(2):
            rows = zc[64 * v + 32 * h : 64 * v + 32 * h + 32, :]
            parts.append(dot1(qz[v], stacked(rows)).reshape(32, 1, 8, 128))
        planes = jnp.concatenate(parts, axis=1).reshape(512, 128)
        copies[v].wait()
        at = pl.ds(512 * v, 512)
        v2[at, :] = vy[at, :] - planes


def last_body(v2, *refs):
    zr, (ny, qzy, qy, out_far, fin, out, sem) = refs[:8], refs[8:]
    stats = merged_stats([r[80:88, :] for r in zr])
    lane = iota((8, 128), 1)
    step = COURANT / jnp.max(jnp.where(lane == VARS, stats, 0.0))
    norm = jnp.sqrt(stats * (1.0 / 16777216.0))
    for v in range(VARS):
        fin[v] = jnp.max(jnp.where(lane == v, norm, 0.0))
    copies = []
    for v in range(VARS):
        table = ny[v]
        crossed = jnp.concatenate(
            [small_solve(table, [x[16 * v + 4 * r : 16 * v + 4 * r + 4, :] for x in zr])[0:4] for r in range(4)], axis=0
        )
        lines = dot1(qzy[v], stacked(crossed))
        for t in range(4):
            at = pl.ds(512 * v + 128 * t, 128)
            out[at, :] = step * (v2[at, :] + dot1(qy[v], stacked(lines[32 * t : 32 * t + 32])))
        at = pl.ds(512 * v, 512)
        copies.append(pltpu.make_async_copy(out.at[at], out_far.at[at], sem.at[v]))
        copies[v].start()
    for c in copies:
        c.wait()


def handed(x, axis):
    return lax.all_to_all(x, axis, 0, 0, tiled=True)


def shifted(x, axis, by):
    size = lax.axis_size(axis)
    return lax.ppermute(x, axis, [(i, (i + by) % size) for i in range(size)])


def swapped(x, axis, k):
    return lax.ppermute(x, axis, [(i, i ^ k) for i in range(lax.axis_size(axis))])


def step(flow_state, advection, inverse_x, inverse_y, inverse_z, reduced_x, reduced_y, reduced_z):
    u = flow_state.reshape(2560, 128)
    xlo, xhi, ylo, yhi, zlo, zhi = call(
        faces_body, [((16, 512), F32)] * 2 + [((320, 128), F32)] * 2 + [((160, 128), F32)] * 2, (u,)
    )
    from_zlo, from_zhi = shifted(zhi, "gz", 1), shifted(zlo, "gz", -1)
    from_ylo, from_yhi = shifted(yhi, "gy", 1), shifted(ylo, "gy", -1)
    from_xlo, from_xhi = shifted(xhi, "gx", 1), shifted(xlo, "gx", -1)
    ay, az = call(solve_tables_body, [((5, 128, 384), BF16), ((5, 256, 768), BF16)], (inverse_y, inverse_z))
    w, bx, qx = call(
        residual_body,
        [((2560, 128), F32), ((24, 512), F32), ((32, 128), F32)],
        (u, from_xlo, from_xhi, from_ylo, from_yhi, from_zlo, from_zhi, xlo, xhi, inverse_x, ay, az),
        scratch=[
            ((180, 32, 128), F32),
            ((160, 32, 128), F32),
            ((170, 16, 128), F32),
            ((160, 16, 128), F32),
            ((512, 128), F32),
            ((512, 128), F32),
            ((128, 512), F32),
        ],
    )
    pieces = [bx] + [shifted(bx, "gx", k) for k in (1, 2, 3)]
    nx, ty, tz, my, mz, ny, qy, qz, qzy = call(
        window_tables_body,
        [
            ((32, 384), BF16),
            ((5, 32, 96), BF16),
            ((5, 32, 96), BF16),
            ((5, 32, 432), BF16),
            ((5, 32, 432), BF16),
            ((5, 16, 96), BF16),
            ((5, 128, 96), BF16),
            ((5, 256, 96), BF16),
            ((5, 128, 48), BF16),
        ],
        (advection, reduced_x, reduced_y, reduced_z, inverse_y, inverse_z),
        scratch=[((32, 256), F32)],
        smem=(0,),
    )
    big, tall, flat = ((2560, 128), F32), ((8, 168, 128), F32), ((320, 128), F32)
    v1, zp, mine, pair, *chips = call(
        spread_body,
        [big, tall, ((160, 128), F32)] + [flat] * 4,
        (w, *pieces, nx, qx, ty, tz),
        scratch=[big, tall, ((128, 512), F32)],
        far_out=(0, 1),
        sems=11,
    )
    zr = handed(zp, "gz").reshape(1344, 128)
    lines = [swapped(pair, "gy", 1)]
    for j in (1, 2, 3):
        lines.append(swapped(chips[j - 1], "gy", 2 * j))
        lines.append(swapped(lines[-1], "gy", 1))
    down, up = call(own_body, [flat, flat], (v1, ty), scratch=[big], far=(0,), sems=5)
    lines = [down, *lines, up]
    (vy,) = call(
        middle_y_body,
        [big],
        (v1, my, qy, *lines),
        scratch=[big, big],
        far=(0,),
        far_out=(0,),
        sems=10,
    )
    zy, zc = call(
        cross_body, [((88, 128), F32), ((320, 128), F32)], (zr, mine, mz, vy), far=(3,)
    )
    crossed = [zy, swapped(zy, "gy", 1)]
    for k in (2, 4, 6):
        crossed.append(swapped(zy, "gy", k))
        crossed.append(swapped(crossed[-1], "gy", 1))
    (v2,) = call(middle_z_body, [big], (vy, zc, qz), scratch=[big], far=(0,), sems=5)
    out, fin = call(
        last_body,
        [((2560, 128), F32), ((VARS,), F32)],
        (v2, *crossed, ny, qzy, qy),
        scratch=[((2560, 128), F32)],
        far_out=(0,),
        smem_out=(1,),
        sems=5,
    )
    return out.reshape(5, 32, 16, 128), fin


def solution(mesh):
    spec = P(None, "gz", "gy", "gx")
    return jax.shard_map(
        step,
        mesh=mesh,
        in_specs=(spec, P(), P(), P(), P(), P(), P(), P()),
        out_specs=(spec, P()),
        check_vma=False,
    )
```

```python
import jax
import jax.numpy as jnp
from jax import lax
from jax.experimental import pallas as pl
from jax.experimental.pallas import tpu as pltpu
from jax.sharding import PartitionSpec as P


VARS = 5
F32 = jnp.float32
BF16 = jnp.bfloat16
DAMP = 0.0625
COURANT = 8000.0
VMEM = pltpu.VMEM
NN = (((1,), (0,)), ((), ()))


def iota(shape, dim):
    return lax.broadcasted_iota(jnp.int32, shape, dim)


def picks(shape, cond):
    return jnp.where(cond(iota(shape, 0), iota(shape, 1)), 1.0, 0.0).astype(BF16)


def split(x):
    hi = x.astype(BF16)
    return hi, (x - hi.astype(F32)).astype(BF16)


def dot1(a, b, dims=NN):
    return lax.dot_general(a, b, dims, preferred_element_type=F32)


def stacked(x):
    hi, lo = split(x)
    return jnp.concatenate([hi, hi, lo], axis=0)


def small_solve(table, pieces):
    return dot1(table, stacked(jnp.concatenate(pieces, axis=0)))


def call(body, out, args, scratch=(), far=(), smem=(), far_out=(), smem_out=(), sems=0, limit=24, flops=1_000_000):
    def spec(k, places):
        if k in smem and places is far:
            return pl.BlockSpec(memory_space=pltpu.SMEM)
        return pl.BlockSpec(memory_space=pltpu.HBM if k in places else VMEM)

    size = sum(a.size * a.dtype.itemsize for a in args)
    shapes = [VMEM(*t) for t in scratch]
    if sems:
        shapes.append(pltpu.SemaphoreType.DMA((sems,)))
    return pl.pallas_call(
        body,
        out_shape=[jax.ShapeDtypeStruct(*o) for o in out],
        in_specs=[spec(k, far) for k in range(len(args))],
        out_specs=[
            pl.BlockSpec(memory_space=pltpu.SMEM if k in smem_out else pltpu.HBM if k in far_out else VMEM)
            for k in range(len(out))
        ],
        scratch_shapes=shapes,
        compiler_params=pltpu.CompilerParams(vmem_limit_bytes=limit * 1024 * 1024),
        cost_estimate=pl.CostEstimate(flops=flops, bytes_accessed=size, transcendentals=0),
    )(*args)


def spread(left, parts, right, keep=None):
    wide = [dot1(dot1(left, part).astype(BF16), right) for part in parts]
    if keep is not None:
        wide = [jnp.where(keep, x, 0.0) for x in wide]
    return [x.astype(BF16) for x in wide]


def masked(shape, cond):
    return cond(iota(shape, 0), iota(shape, 1))


def put(ref, v, halves):
    hi, lo = halves
    k = hi.shape[1]
    ref[v, :, 0:k] = hi
    ref[v, :, k : 2 * k] = lo
    ref[v, :, 2 * k : 3 * k] = hi


def solve_tables_body(invy, invz, ay, az):
    y_left = picks((128, 16), lambda a, k: (a & 15) == k)
    y_right = picks((16, 128), lambda k, c: k == (c & 15))
    y_same = masked((128, 128), lambda a, c: (a >> 4) == (c >> 4))
    z_left = picks((256, 32), lambda a, k: (a >> 3) == k)
    z_right = picks((32, 256), lambda k, c: k == (c >> 3))
    z_same = masked((256, 256), lambda a, c: (a & 7) == (c & 7))
    for v in range(VARS):
        put(ay, v, spread(y_left, split(invy[v]), y_right, y_same))
        put(az, v, spread(z_left, split(invz[v]), z_right, z_same))


def first_off(r):
    return r - 2 + 4 * (r >> 1)


def second_off(r):
    return jnp.where(r == 0, -1, jnp.where(r == 3, 4, -4096))


def near(chosen, red, row, speed):
    hi, lo = split(red)
    both = dot1(chosen, hi) + dot1(chosen, lo)
    rows = both.shape[0] // 2
    other = jnp.where(row == 0, -0.5 * speed - 2.0, jnp.where(row == 3, 0.5 * speed - 2.0, 0.0))
    return 0.5 * both[0:rows] + other * both[rows:]


def exact(a, b):
    return lax.dot_general(a, b, NN, precision=lax.Precision.HIGHEST, preferred_element_type=F32)


def send_tables(adv, redx, redy, redz, nx, ty, tz):
    ix, iy, iz = lax.axis_index("gx"), lax.axis_index("gy"), lax.axis_index("gz")
    same = masked((32, 32), lambda a, c: (a & 7) == (c & 7))
    for out, red, at in ((ty, redy, iy), (tz, redz, iz)):
        left = picks((32, 32), lambda a, k: k == 4 * at + (a >> 3))
        right = picks((32, 32), lambda k, c: k == 4 * at + (c >> 3))
        for v in range(VARS):
            put(out, v, spread(left, split(red[v]), right, same))
    total = None
    row = (iota((32, 16), 0) & 3) ^ 2
    for v in range(VARS):
        chosen = jnp.concatenate(
            [
                picks((32, 16), lambda a, k, f=f: ((a >> 2) == v) & (k == 4 * ix + f((a & 3) ^ 2)))
                for f in (first_off, second_off)
            ],
            axis=0,
        )
        term = near(chosen, redx[v], row, adv[0, v])
        total = term if total is None else total + term
    right = picks((16, 128), lambda k, c: k == 4 * ((ix + 4 - (c >> 5)) & 3) + ((c & 3) ^ 2))
    same = masked((32, 128), lambda a, c: (a >> 2) == ((c >> 2) & 7))
    hi, lo = [jnp.where(same, dot1(part, right), 0.0).astype(BF16) for part in split(total)]
    nx[:, 0:128] = hi
    nx[:, 128:256] = lo
    nx[:, 256:384] = hi


def take_tables(adv, redy, redz, my, mz, ny, wide):
    row, lane = iota((32, 160), 0), iota((32, 160), 1)
    block, first = (lane >> 2) & 7, row - (lane & 28)
    low = (iota((8, 160), 0) & 3) < 2
    same = jnp.where((iota((160, 160), 0) >> 2) == (iota((160, 160), 1) >> 2), 1.0, 0.0)
    keep = masked((32, 432), lambda a, c: (a & 7) == (c & 7))
    left = picks((32, 8), lambda a, k: k == (a >> 3))
    third = iota((32, 432), 1)
    third, spot = jnp.where(third < 144, 0, jnp.where(third < 288, 1, 2)), third
    spot = (spot - 144 * third) >> 3
    spot = jnp.where(iota((32, 432), 0) == spot, 1.0, 0.0)
    ends, inner = jnp.where(third == 1, 0.0, spot).astype(BF16), jnp.where(third == 1, spot, 0.0).astype(BF16)
    source, column = iota((640, 160), 0), iota((640, 160), 1)
    part = jnp.where(source < 160, 0, jnp.where(source < 320, 1, jnp.where(source < 480, 2, 3)))
    inside = source - 160 * part
    for out, red, d, axis in ((my, redy, 1, "gy"), (mz, redz, 2, "gz")):
        at = lax.axis_index(axis)
        flip = at if axis == "gy" else 0
        for v in range(VARS):
            wide[:, 32 * v : 32 * v + 32] = red[v]
        table = wide[:, 0:160]
        start = jnp.where(block < at, 2, 0)
        here = block[0:8] == at

        def line(which):
            return jnp.sum(jnp.where(which, table, 0.0), axis=0, keepdims=True)

        a0, a1 = line(first == start), line(first == start + 1)
        e0, e1 = line(first == 2), line(first == 3)
        blank = jnp.zeros((2, 160), F32)
        sums = exact(jnp.concatenate([a0 * a0, a0 * a1, a1 * a1, e0 * e0, e0 * e1, e1 * e1, blank], axis=0), same)

        def dual(u0, u1, g):
            scale = 1.0 / (g[0:1] * g[2:3] - g[1:2] * g[1:2])
            return (g[2:3] * u0 - g[1:2] * u1) * scale, (g[0:1] * u1 - g[1:2] * u0) * scale

        p0, p1 = dual(a0, a1, sums[0:3])
        f0, f1 = dual(e0, e1, sums[3:6])
        chosen = jnp.concatenate(
            [picks((8, 32), lambda a, k, f=f: k == 4 * at + f(a & 3)) for f in (first_off, second_off)], axis=0
        )
        speed = jnp.zeros((8, 160), F32)
        for v in range(VARS):
            speed = jnp.where((iota((8, 160), 1) >> 5) == v, adv[d, v], speed)
        needed = near(chosen, table, iota((8, 160), 0) & 3, speed)
        sent = jnp.where(here & ~low, 0.0, needed)
        own = jnp.where(here & ~low, needed, 0.0)
        place = jnp.where(part < 2, 2 * (((inside >> 2) & 7) ^ flip), 14) + part
        gather = jnp.where(column == (inside & 224) + place, 1.0, 0.0)
        found = exact(jnp.concatenate([sent * p0, sent * p1, own * f0, own * f1], axis=1), gather)
        hi, lo = [dot1(left, x).astype(BF16) for x in split(found)]
        for v in range(VARS):
            at_v = slice(32 * v, 32 * v + 32)
            out[v] = jnp.where(keep, dot1(hi[:, at_v], ends) + dot1(lo[:, at_v], inner), 0.0).astype(BF16)
        if axis == "gy":
            wanted = iota((32, 96), 0) == 4 * (at ^ ((iota((32, 96), 1) >> 2) & 7)) + (iota((32, 96), 1) & 3)
            second = (iota((32, 96), 1) >> 5) == 1
            y_ends = jnp.where(wanted & ~second, 1.0, 0.0).astype(BF16)
            y_inner = jnp.where(wanted & second, 1.0, 0.0).astype(BF16)
            hi, lo = [jnp.concatenate([x, x], axis=0) for x in split(needed)]
            for v in range(VARS):
                at_v = slice(32 * v, 32 * v + 32)
                ny[v] = (dot1(hi[:, at_v], y_ends) + dot1(lo[:, at_v], y_inner)).astype(BF16)


def window_tables_body(adv, redx, redy, redz, invy, invz, nx, ty, tz, my, mz, ny, qy, qz, qzy, wide):
    send_tables(adv, redx, redy, redz, nx, ty, tz)
    take_tables(adv, redy, redz, my, mz, ny, wide)
    column_tables(invy, invz, qy, qz, qzy)


def column_tables(invy, invz, qy, qz, qzy):
    y_left = picks((128, 16), lambda a, k: (a & 15) == k)
    y_right = picks((16, 32), lambda k, c: k == (c >> 3) + 12 * (c >> 4))
    y_same = masked((128, 32), lambda a, c: (a >> 4) == (c & 7))
    z_left = picks((256, 32), lambda a, k: (a >> 3) == k)
    z_right = picks((32, 32), lambda k, c: k == (c >> 3) + 28 * (c >> 4))
    z_same = masked((256, 32), lambda a, c: (a & 7) == (c & 7))
    zy_left = picks((128, 32), lambda a, k: k == 8 * (a >> 5) + (a & 7))
    zy_right = picks((32, 16), lambda k, c: k == (c >> 2) + 28 * (c >> 3))
    zy_same = masked((128, 16), lambda a, c: ((a >> 3) & 3) == (c & 3))
    for v in range(VARS):
        put(qy, v, spread(y_left, split(invy[v]), y_right, y_same))
        parts = split(invz[v])
        put(qz, v, spread(z_left, parts, z_right, z_same))
        put(qzy, v, spread(zy_left, parts, zy_right, zy_same))


def faces_body(u, xlo, xhi, ylo, yhi, zlo, zhi):
    lane = iota((512, 128), 1)
    wide = jnp.zeros((512, 128), F32)
    for v in range(VARS):
        block = u[512 * v : 512 * v + 512, :]
        low = pltpu.roll(block, 2 * v, 1) if v else block
        wide = jnp.where((lane >> 1) == v, low, wide)
        wide = jnp.where((lane >> 1) == 8 + v, pltpu.roll(block, 18 + 2 * v, 1), wide)
        for j in range(2):
            at = 32 * (2 * v + j)
            ylo[at : at + 32, :] = u[pl.ds(512 * v + j, 32, stride=16), :]
            yhi[at : at + 32, :] = u[pl.ds(512 * v + 14 + j, 32, stride=16), :]
        zlo[32 * v : 32 * v + 32, :] = u[512 * v : 512 * v + 32, :]
        zhi[32 * v : 32 * v + 32, :] = u[512 * v + 480 : 512 * v + 512, :]
    turned = wide.T
    xlo[...] = turned[0:16]
    xhi[...] = turned[16:32]


def primitives(u):
    inverse = 1.0 / u[0]
    velocity = [u[1 + k] * inverse for k in range(3)]
    kinetic = 0.5 * (velocity[0] * velocity[0] + velocity[1] * velocity[1] + velocity[2] * velocity[2])
    internal = jnp.maximum(u[4] * inverse - kinetic, 0.25)
    return velocity, internal, 0.4 * u[0] * internal


def flux(u, velocity, pressure, d):
    w = velocity[d]
    out = [u[1 + d]]
    for k in range(3):
        moment = u[1 + k] * w
        out.append(moment + pressure if k == d else moment)
    out.append((u[4] + pressure) * w)
    return out


def stats_row(shape, sums, top):
    lane = iota(shape, len(shape) - 1)
    row = jnp.where(lane == VARS, top, 0.0)
    for v in range(VARS):
        row = jnp.where(lane == v, sums[v], row)
    return row


def merged_stats(rows):
    lane = iota(rows[0].shape, 1)
    total, top = rows[0], rows[0]
    for row in rows[1:]:
        total, top = total + row, jnp.maximum(top, row)
    return jnp.where(lane < VARS, total, top)


def residual_body(
    u, xlo, xhi, ylo, yhi, zlo, zhi, own_lo, own_hi, invx, ay, az, w, bx, qx, pad, fy, fz, res, fix, half, edge
):
    def fill(z, carry):
        for v in range(VARS):
            pad[36 * v + 2 + z, 8:24, :] = u[pl.ds(pl.multiple_of(512 * v + 16 * z, 16), 16), :]
        return carry

    lax.fori_loop(0, 32, fill, 0)
    rows = pad.reshape(180 * 32, 128)
    for v in range(VARS):
        for k in range(2):
            pad[36 * v + k, 8:24, :] = zlo[32 * v + 16 * k : 32 * v + 16 * k + 16, :]
            pad[36 * v + 34 + k, 8:24, :] = zhi[32 * v + 16 * k : 32 * v + 16 * k + 16, :]
            at = 32 * (2 * v + k)
            rows[pl.ds(32 * (36 * v + 2) + 6 + k, 32, stride=32), :] = ylo[at : at + 32, :]
            rows[pl.ds(32 * (36 * v + 2) + 24 + k, 32, stride=32), :] = yhi[at : at + 32, :]

    edge[...] = jnp.zeros_like(edge)

    def line(ref, j):
        return [ref[2 * v + j : 2 * v + j + 1, :] for v in range(VARS)]

    def fx(u):
        velocity, _, pressure = primitives(u)
        return flux(u, velocity, pressure, 0)

    l2, l1, h1, h2 = line(xlo, 0), line(xlo, 1), line(xhi, 0), line(xhi, 1)
    o0, o1, p1, p0 = line(own_lo, 0), line(own_lo, 1), line(own_hi, 0), line(own_hi, 1)
    fl, fp, fh, fo = fx(l1), fx(p0), fx(h1), fx(o0)
    for v in range(VARS):
        dl, dh = l1[v] - p0[v], h1[v] - o0[v]
        edge[4 * v : 4 * v + 1, :] = -DAMP * dh
        edge[4 * v + 1 : 4 * v + 2, :] = -0.5 * (fh[v] - fo[v]) + 4.0 * DAMP * dh - DAMP * (h2[v] - o1[v])
        edge[4 * v + 2 : 4 * v + 3, :] = 0.5 * (fl[v] - fp[v]) + 4.0 * DAMP * dl - DAMP * (l2[v] - p1[v])
        edge[4 * v + 3 : 4 * v + 4, :] = -DAMP * dl
    fix[...] = edge[...].T

    for z in (-1, 32):
        c = [pad[36 * v + 2 + z, 8:24, :] for v in range(VARS)]
        velocity, _, pressure = primitives(c)
        for v, f in enumerate(flux(c, velocity, pressure, 2)):
            fz[34 * v + 1 + z] = f

    def plane(z, top):
        full = [pad[36 * v + 2 + z] for v in range(VARS)]
        velocity, internal, pressure = primitives(full)
        for v, f in enumerate(flux(full, velocity, pressure, 1)):
            fy[32 * v + z] = f
        c = [f[8:24] for f in full]
        velocity, internal, pressure = [f[8:24] for f in velocity], internal[8:24], pressure[8:24]
        for v, f in enumerate(flux(c, velocity, pressure, 2)):
            fz[34 * v + 1 + z] = f
        for v, f in enumerate(flux(c, velocity, pressure, 0)):
            damped = (4.0 * DAMP) * c[v]
            res[32 * v + z] = (
                pltpu.roll(damped - 0.5 * f, 127, 1)
                + pltpu.roll(damped + 0.5 * f, 1, 1)
                - DAMP * (pltpu.roll(c[v], 126, 1) + pltpu.roll(c[v], 2, 1))
                - (18.0 * DAMP) * c[v]
            )
        speed = jnp.abs(velocity[0]) + jnp.abs(velocity[1]) + jnp.abs(velocity[2])
        return jnp.maximum(top, speed + jnp.sqrt((3.0 * 1.4 * 0.4) * internal))

    top = lax.fori_loop(0, 32, plane, jnp.zeros((16, 128), F32), unroll=4)

    lane = iota((16, 128), 1)
    edges = (lane < 2) | (lane >= 126)

    def finish(z, sums):
        out = []
        fixes = fix[pl.ds(pl.multiple_of(16 * z, 16), 16), :]
        for v in range(VARS):
            at = 36 * v + 2 + z
            ones = (pad[at, 7:23, :] + pad[at, 9:25, :]) + (pad[at - 1, 8:24, :] + pad[at + 1, 8:24, :])
            twos = (pad[at, 6:22, :] + pad[at, 10:26, :]) + (pad[at - 2, 8:24, :] + pad[at + 2, 8:24, :])
            steep = (fy[32 * v + z, 7:23, :] - fy[32 * v + z, 9:25, :]) + (fz[34 * v + z] - fz[34 * v + 2 + z])
            value = res[32 * v + z] + 0.5 * steep + (4.0 * DAMP) * ones - DAMP * twos
            value = value + jnp.where(edges, pltpu.roll(fixes, (126 - 4 * v) & 127, 1), 0.0)
            res[32 * v + z] = value
            out.append(sums[v] + value * value)
        return tuple(out)

    sums = lax.fori_loop(0, 32, finish, tuple(jnp.zeros((16, 128), F32) for _ in range(VARS)), unroll=2)

    qx[...] = jnp.zeros_like(qx)
    for v in range(VARS):
        turned = invx[v].T
        qx[4 * v : 4 * v + 2, :] = turned[126:128]
        qx[4 * v + 2 : 4 * v + 4, :] = turned[0:2]
        hi, lo = split(res[pl.ds(32 * v, 32)].reshape(512, 128))
        half[...] = dot1(jnp.concatenate([hi, lo, hi], axis=1), stacked(turned))
        for g in range(4):
            half[128 * g : 128 * g + 128, :] = dot1(ay[v], stacked(half[128 * g : 128 * g + 128, :]))
        field = half[...].reshape(32, 2, 8, 128)
        parts = [dot1(az[v], stacked(field[:, h].reshape(256, 128))).reshape(32, 1, 8, 128) for h in range(2)]
        w[pl.ds(pl.multiple_of(512 * v, 512), 512), :] = jnp.concatenate(parts, axis=1).reshape(512, 128)
    lane = iota((512, 128), 1)
    wide = jnp.zeros((512, 128), F32)
    for v in range(VARS):
        wide = jnp.where((lane >> 2) == v, pltpu.roll(w[512 * v : 512 * v + 512, :], 2 + 4 * v, 1), wide)
    turned = wide.T
    bx[...] = turned[0:24]
    bx[20:21, :] = stats_row((1, 512), [jnp.sum(s) for s in sums], jnp.max(top))


def spread_body(w, b0, b1, b2, b3, nx, qx, tz, *rest):
    far, mine, (v1, zp, wide, sem) = rest[:2], rest[2], rest[3:]
    iz = lax.axis_index("gz")
    blank = jnp.zeros((8, 512), F32)
    pieces = [b0, b1, b2, b3]
    data = jnp.concatenate([t for p in pieces for t in (p[...], blank)], axis=0)
    wide[...] = jnp.zeros_like(wide)
    wide[0:32, :] = dot1(nx[...], stacked(data))
    hi, lo = split(wide[...].T[:, 0:32])
    turned = jnp.concatenate([hi, lo, hi], axis=1)
    copies = []
    for v in range(VARS):
        at = pl.ds(512 * v, 512)
        hi, lo = split(jnp.where((iota((32, 128), 0) >> 2) == v, qx[...], 0.0))
        v1[at, :] = w[at, :] - dot1(turned, jnp.concatenate([hi, hi, lo], axis=0))
        copies.append(pltpu.make_async_copy(v1.at[at], far[0].at[at], sem.at[v]))
        copies[-1].start()
        for h in range(2):
            ends = [v1[512 * v + 16 * z + 8 * h : 512 * v + 16 * z + 8 * h + 8, :] for z in (0, 1, 30, 31)]
            sent = small_solve(tz[v], ends)
            at = 16 * (2 * v + h)
            mine[at : at + 16, :] = sent[16:32]
            for p in range(8):
                zp[p, at : at + 16, :] = jnp.where(p <= iz, sent[0:16], sent[16:32])
        at = pl.ds(32 * v, 32)
        copies.append(pltpu.make_async_copy(zp.at[:, at], far[1].at[:, at], sem.at[5 + v]))
        copies[-1].start()
    stats = jnp.broadcast_to(merged_stats([p[20:21, 0:128] for p in pieces]), (8, 128))
    for p in range(8):
        zp[p, 160:168, :] = stats
    at = pl.ds(160, 8)
    copies.append(pltpu.make_async_copy(zp.at[:, at], far[1].at[:, at], sem.at[10]))
    copies[-1].start()
    for c in copies:
        c.wait()


def cross_body(zr, mine, mz, *refs):
    zy, zc = refs[-2:]
    for v in range(VARS):
        for h in range(2):
            at = 16 * (2 * v + h)
            got = [zr[168 * q + at : 168 * q + at + 16, :] for q in range(8)] + [mine[at : at + 16, :]]
            zc[2 * at : 2 * at + 32, :] = small_solve(mz[v], got)
        for j, (h, y) in enumerate(((0, 0), (0, 1), (1, 6), (1, 7))):
            zy[pl.ds(16 * v + j, 4, stride=4), :] = zc[pl.ds(32 * (2 * v + h) + y, 4, stride=8), :]
    zy[80:88, :] = merged_stats([zr[168 * q + 160 : 168 * q + 168, :] for q in range(8)])


def send_y_body(v1_far, ty, down, up, *rest):
    towards, (v1, sem) = rest[:4], rest[4:]
    me = lax.axis_index("gy")
    ups = [(me & 1) == 0] + [((me >> 1) ^ j) > (me >> 1) for j in (1, 2, 3)]
    copies = []
    for v in range(VARS):
        at = pl.ds(512 * v, 512)
        copies.append(pltpu.make_async_copy(v1_far.at[at], v1.at[at], sem.at[v]))
        copies[v].start()
    for v in range(VARS):
        copies[v].wait()
        for t in range(4):
            sent = small_solve(ty[v], [v1[pl.ds(512 * v + 128 * t + y, 8, stride=16), :] for y in (0, 1, 14, 15)])
            at = 16 * (4 * v + t)
            down[at : at + 16, :] = sent[0:16]
            up[at : at + 16, :] = sent[16:32]
            for choice, out in zip(ups, towards):
                out[at : at + 16, :] = jnp.where(choice, sent[16:32], sent[0:16])


def middle_y_body(v1_far, my, qy, *refs):
    lines, (vy_far, v1, vy, sem) = refs[:9], refs[9:]
    copies, puts = [], []
    for v in range(VARS):
        at = pl.ds(512 * v, 512)
        copies.append(pltpu.make_async_copy(v1_far.at[at], v1.at[at], sem.at[v]))
        puts.append(pltpu.make_async_copy(vy.at[at], vy_far.at[at], sem.at[5 + v]))
        copies[v].start()
    for v in range(VARS):
        copies[v].wait()
        for t in range(4):
            at = 16 * (4 * v + t)
            found = small_solve(my[v], [x[at : at + 16, :] for x in lines])
            at = pl.ds(512 * v + 128 * t, 128)
            vy[at, :] = v1[at, :] - dot1(qy[v], stacked(found))
        puts[v].start()
    for c in puts:
        c.wait()


def middle_z_body(vy_far, zc, qz, v2, vy, sem):
    copies = []
    for v in range(VARS):
        at = pl.ds(512 * v, 512)
        copies.append(pltpu.make_async_copy(vy_far.at[at], vy.at[at], sem.at[v]))
        copies[v].start()
    for v in range(VARS):
        parts = []
        for h in range(2):
            rows = zc[64 * v + 32 * h : 64 * v + 32 * h + 32, :]
            parts.append(dot1(qz[v], stacked(rows)).reshape(32, 1, 8, 128))
        planes = jnp.concatenate(parts, axis=1).reshape(512, 128)
        copies[v].wait()
        at = pl.ds(512 * v, 512)
        v2[at, :] = vy[at, :] - planes


def last_body(v2, *refs):
    zr, (ny, qzy, qy, out_far, fin, out, sem) = refs[:8], refs[8:]
    stats = merged_stats([r[80:88, :] for r in zr])
    lane = iota((8, 128), 1)
    step = COURANT / jnp.max(jnp.where(lane == VARS, stats, 0.0))
    norm = jnp.sqrt(stats * (1.0 / 16777216.0))
    for v in range(VARS):
        fin[v] = jnp.max(jnp.where(lane == v, norm, 0.0))
    copies = []
    for v in range(VARS):
        table = ny[v]
        crossed = jnp.concatenate(
            [small_solve(table, [x[16 * v + 4 * r : 16 * v + 4 * r + 4, :] for x in zr])[0:4] for r in range(4)], axis=0
        )
        lines = dot1(qzy[v], stacked(crossed))
        for t in range(4):
            at = pl.ds(512 * v + 128 * t, 128)
            out[at, :] = step * (v2[at, :] + dot1(qy[v], stacked(lines[32 * t : 32 * t + 32])))
        at = pl.ds(512 * v, 512)
        copies.append(pltpu.make_async_copy(out.at[at], out_far.at[at], sem.at[v]))
        copies[v].start()
    for c in copies:
        c.wait()


def handed(x, axis):
    return lax.all_to_all(x, axis, 0, 0, tiled=True)


def shifted(x, axis, by):
    size = lax.axis_size(axis)
    return lax.ppermute(x, axis, [(i, (i + by) % size) for i in range(size)])


def swapped(x, axis, k):
    return lax.ppermute(x, axis, [(i, i ^ k) for i in range(lax.axis_size(axis))])


def step(flow_state, advection, inverse_x, inverse_y, inverse_z, reduced_x, reduced_y, reduced_z):
    u = flow_state.reshape(2560, 128)
    xlo, xhi, ylo, yhi, zlo, zhi = call(
        faces_body, [((16, 512), F32)] * 2 + [((320, 128), F32)] * 2 + [((160, 128), F32)] * 2, (u,)
    )
    from_zlo, from_zhi = shifted(zhi, "gz", 1), shifted(zlo, "gz", -1)
    from_ylo, from_yhi = shifted(yhi, "gy", 1), shifted(ylo, "gy", -1)
    from_xlo, from_xhi = shifted(xhi, "gx", 1), shifted(xlo, "gx", -1)
    ay, az = call(solve_tables_body, [((5, 128, 384), BF16), ((5, 256, 768), BF16)], (inverse_y, inverse_z))
    w, bx, qx = call(
        residual_body,
        [((2560, 128), F32), ((24, 512), F32), ((32, 128), F32)],
        (u, from_xlo, from_xhi, from_ylo, from_yhi, from_zlo, from_zhi, xlo, xhi, inverse_x, ay, az),
        scratch=[
            ((180, 32, 128), F32),
            ((160, 32, 128), F32),
            ((170, 16, 128), F32),
            ((160, 16, 128), F32),
            ((512, 128), F32),
            ((512, 128), F32),
            ((128, 512), F32),
        ],
    )
    pieces = [bx] + [shifted(bx, "gx", k) for k in (1, 2, 3)]
    nx, ty, tz, my, mz, ny, qy, qz, qzy = call(
        window_tables_body,
        [
            ((32, 384), BF16),
            ((5, 32, 96), BF16),
            ((5, 32, 96), BF16),
            ((5, 32, 432), BF16),
            ((5, 32, 432), BF16),
            ((5, 16, 96), BF16),
            ((5, 128, 96), BF16),
            ((5, 256, 96), BF16),
            ((5, 128, 48), BF16),
        ],
        (advection, reduced_x, reduced_y, reduced_z, inverse_y, inverse_z),
        scratch=[((32, 256), F32)],
        smem=(0,),
    )
    big, tall, flat = ((2560, 128), F32), ((8, 168, 128), F32), ((320, 128), F32)
    v1, zp, mine = call(
        spread_body,
        [big, tall, ((160, 128), F32)],
        (w, *pieces, nx, qx, tz),
        scratch=[big, tall, ((128, 512), F32)],
        far_out=(0, 1),
        sems=11,
    )
    zr = handed(zp, "gz").reshape(1344, 128)
    down, up, pair, *chips = call(send_y_body, [flat] * 6, (v1, ty), scratch=[big], far=(0,), sems=5)
    lines = [swapped(pair, "gy", 1)]
    for j in (1, 2, 3):
        lines.append(swapped(chips[j - 1], "gy", 2 * j))
        lines.append(swapped(lines[-1], "gy", 1))
    lines = [down, *lines, up]
    (vy,) = call(
        middle_y_body,
        [big],
        (v1, my, qy, *lines),
        scratch=[big, big],
        far=(0,),
        far_out=(0,),
        sems=10,
    )
    zy, zc = call(
        cross_body, [((88, 128), F32), ((320, 128), F32)], (zr, mine, mz, vy), far=(3,)
    )
    crossed = [zy, swapped(zy, "gy", 1)]
    for k in (2, 4, 6):
        crossed.append(swapped(zy, "gy", k))
        crossed.append(swapped(crossed[-1], "gy", 1))
    (v2,) = call(middle_z_body, [big], (vy, zc, qz), scratch=[big], far=(0,), sems=5)
    out, fin = call(
        last_body,
        [((2560, 128), F32), ((VARS,), F32)],
        (v2, *crossed, ny, qzy, qy),
        scratch=[((2560, 128), F32)],
        far_out=(0,),
        smem_out=(1,),
        sems=5,
    )
    return out.reshape(5, 32, 16, 128), fin


def solution(mesh):
    spec = P(None, "gz", "gy", "gx")
    return jax.shard_map(
        step,
        mesh=mesh,
        in_specs=(spec, P(), P(), P(), P(), P(), P(), P()),
        out_specs=(spec, P()),
        check_vma=False,
    )
```
